256 devices in a mesh: obs: 64 (over z, y, core), rep: 4 (over x).
Axes of the slice: x: 4, y: 4, z: 8, core: 2. Of those that a mesh axis runs over, the one named last changes fastest.
Arguments:
- jacobians: float32 [18, 8388608], P(None, ('obs', 'rep')), may hold values from -3 to 3
- residuals: float32 [2, 8388608], P(None, ('obs', 'rep')), may hold values from -6 to 6
- camera_local: int32 [8388608], P(('obs', 'rep')), may hold values from 0 to 1023
- bucket_counts: int32 [256, 64], P(('obs', 'rep')), may hold values from 1 to 512, as said below
- camera_map: int32 [65536], replicated, may hold values from 0 to 65535, each once
Outputs:
- gradient: float32 [9, 65536], replicated
- camera_blocks: float32 [81, 65536], P(None, 'obs')
The draws below stay inside these ranges and needn't reach their ends.
Inputs may be any that keep to these rules, and one draw needn't show every extreme that they name: bucket_counts[s, d] counts the leading live slots of bucket d of source block s; exactly one destination d has all 512 slots live from every source block, and every other bucket has at most 256 live slots. A slot in bucket d names camera slot d * 1024 + camera_local. `camera_map`: each camera id appears once.
All inputs are finite; a program needn't handle non-finite values.
Results may differ from the reference program's by a relative error of at most 0.0003.
Values sent between devices are 32-bit elements; how exact they have to be, the bound alone decides.
A program may use at most 192 MiB of HBM per device.

```python
import math
import jax
import jax.numpy as jnp
import numpy as np
from jax import lax

CAM_DEV = 1024
CAP = 512
CAM = 65536
SLOTS = 8388608
N_OBS = 64
N_REP = 4


def draw_bucket_counts(key, part):
    key_hot = jax.random.fold_in(key, 11)
    key_full = jax.random.fold_in(key, 12)
    key_base = jax.random.fold_in(key, 13)
    hotness = jax.random.randint(key_hot, (N_OBS,), 1, 4)
    full_column = jax.random.randint(key_full, (), 0, N_OBS)
    baseline = jax.random.randint(key_base, (N_OBS * N_REP, N_OBS), CAP // 4, CAP // 2 + 1)
    counts = jnp.minimum(CAP // 2, baseline * hotness[None, :] // 2)
    counts = jnp.maximum(counts, 1)
    column_ids = jnp.arange(N_OBS, dtype=jnp.int32)
    counts = jnp.where(column_ids[None, :] == full_column, CAP, counts)
    return counts.astype(jnp.int32)


def set_ends(drawn, rng, low, largest):
    index_at = [jax.random.randint(jax.random.fold_in(rng, axis), (), 0, length) for axis, length in enumerate(drawn.shape)]
    widest = drawn.shape.index(max(drawn.shape))
    neighbour = index_at[:widest] + [(index_at[widest] + 1) % drawn.shape[widest]] + index_at[widest + 1:]
    return drawn.at[tuple(index_at)].set(low).at[tuple(neighbour)].set(largest)


def block_scale(rng, dims, pieces, smallest, high):
    level, own = 1.0, jax.random.fold_in(rng, 6)
    for dim, shards_of in pieces:
        heights = jnp.exp(jax.random.uniform(jax.random.fold_in(own, dim), (shards_of,), jnp.float32, smallest / len(pieces), high / len(pieces)))
        level = level * jnp.repeat(heights, dims[dim] // shards_of).reshape([-1 if axis == dim else 1 for axis in range(len(dims))])
    return level


def rank_bounds(amount, skew):
    loads = [(1 << 20) // math.isqrt(grade ** skew) + 1 for grade in range(1, amount + 1)]
    scale = 1 + sum(loads) // (1 << 30)
    return np.cumsum(np.array([max(1, weight // scale) for weight in loads]))


def ranked_ids(key, dims, count, lean):
    grid = rank_bounds(count, lean)
    ticket = jax.random.randint(jax.random.fold_in(key, 1), dims, 0, int(grid[count - 1]))
    grade = jnp.searchsorted(jnp.asarray(grid, jnp.int32), ticket, side="right")
    return jax.random.permutation(jax.random.fold_in(key, 2), count)[grade].astype(jnp.int32)


def normal_values(rng, shape, width, most, shards=(), kind=jnp.bfloat16):
    level = block_scale(rng, shape, shards, -0.22, 0.18) if shards else 1.0
    values = jax.random.normal(rng, shape, jnp.float32) * width * level
    return jnp.minimum(jnp.maximum(values, -most), most).astype(kind)


def setup_inputs(seed: int = 0) -> dict:
    key_of = jax.random.split(jax.random.key(seed), 6)
    return {
        "jacobians": normal_values(key_of[0], (18, SLOTS), 0.5, 3.0, ((1, 256),), jnp.float32),
        "residuals": normal_values(key_of[1], (2, SLOTS), 1.0, 6.0, ((1, 256),), jnp.float32),
        "camera_local": set_ends(ranked_ids(key_of[2], (SLOTS,), CAM_DEV, 1), jax.random.fold_in(key_of[2], 3), 0, CAM_DEV - 1).astype(jnp.int32),
        "bucket_counts": draw_bucket_counts(jax.random.fold_in(key_of[5], 71), 0),
        "camera_map": jax.random.permutation(key_of[4], CAM).astype(jnp.int32),
    }


def observation_terms(jacobs, resids):
    leading_row = jacobs[0:9]
    trailing_row = jacobs[9:18]
    gradient_terms = leading_row * resids[0:1] + trailing_row * resids[1:2]
    block_terms = leading_row[:, None] * leading_row[None, :] + trailing_row[:, None] * trailing_row[None, :]
    block_terms = block_terms.reshape((81,) + leading_row.shape[1:])
    return jnp.concatenate([gradient_terms, block_terms], axis=0)


def reference(jacobians, residuals, camera_local, bucket_counts, camera_map):
    sources = N_OBS * N_REP
    columns = N_OBS * CAP
    jac_blocks = jnp.moveaxis(jacobians.reshape(18, sources, columns), 1, 0)
    res_blocks = jnp.moveaxis(residuals.reshape(2, sources, columns), 1, 0)
    cam_blocks = camera_local.reshape(sources, columns)
    position = jnp.arange(columns, dtype=jnp.int32)
    target = position // CAP
    within = position % CAP

    def accumulate(summed, inputs):
        jac_here, res_here, cam_here, count_here = inputs
        live_mask = (within < count_here[target]).astype(jnp.float32)
        obs_terms = observation_terms(jac_here * live_mask, res_here * live_mask)
        segment = (target * CAM_DEV + cam_here).astype(jnp.int32)
        return summed + jax.ops.segment_sum(obs_terms.T, segment, num_segments=CAM), None

    summed, unused = lax.scan(accumulate, jnp.zeros((CAM, 90), jnp.float32), (jac_blocks, res_blocks, cam_blocks, bucket_counts))
    slot_gradient = summed[:, :9].T
    camera_blocks = summed[:, 9:].T
    gradient = jnp.zeros((9, CAM), jnp.float32).at[:, camera_map].set(slot_gradient)
    return gradient, camera_blocks
```

```python
import functools

import jax
import jax.numpy as jnp
from jax import lax
from jax.experimental import pallas as pl
from jax.experimental.pallas import tpu as pltpu
from jax.sharding import PartitionSpec as P

MESH = pl.DeviceIdType.MESH
F32 = jnp.float32
BF16 = jnp.bfloat16
CAP = 512
HALF = 512
ROWS = 56
MSG = 25
VM = functools.partial(pl.BlockSpec, memory_space=pltpu.VMEM)
SM = functools.partial(pl.BlockSpec, memory_space=pltpu.SMEM)


def place():
    obs = lax.axis_index("obs")
    return obs // 8, (obs // 2) % 4, obs % 2, lax.axis_index("rep")


def bucket_of(z, y, core, x):
    return (2 * x + z % 2) * 8 + y * 2 + core


def terms(jac, res):
    j0, j1, r0, r1 = jac[0:9], jac[9:18], res[0:1], res[1:2]

    def turned(j, k):
        return j[0:8] if k == 0 else j[1:9] if k == 1 else jnp.concatenate([j[k:9], j[0 : k - 1]], axis=0)

    rows = [j0[0:8] * turned(j0, k) + j1[0:8] * turned(j1, k) for k in range(5)]
    last0 = jnp.concatenate([j0[8:9], j0[0:4], j0[0:2], r0], axis=0)
    last1 = jnp.concatenate([j1[8:9], j1[0:4], j1[0:2], r1], axis=0)
    rows.append(j0[8:9] * last0 + j1[8:9] * last1)
    rows.append(j0[0:8] * r0 + j1[0:8] * r1)
    return jnp.concatenate(rows, axis=0)


def weighted(jac, res, ids):
    full = terms(jac, res)
    high = full.astype(BF16).astype(F32)
    both = jnp.concatenate([high, full - high], axis=0)
    upper = ids >= HALF
    weights = jnp.concatenate([jnp.where(upper, 0.0, both), jnp.where(upper, both, 0.0)], axis=0)
    ids = jnp.where(upper, ids - HALF, ids)
    rows = lax.broadcasted_iota(jnp.int32, (HALF, ids.shape[1]), 0).astype(F32)
    hot = jnp.where(rows == ids, 1.0, 0.0).astype(BF16)
    return lax.dot_general(hot, weights.astype(BF16), (((1,), (1,)), ((), ())), preferred_element_type=F32)


def unfolded(acc_ref):
    turned = acc_ref[...].T
    low = turned[0:ROWS] + turned[ROWS : 2 * ROWS]
    high = turned[2 * ROWS : 3 * ROWS] + turned[3 * ROWS : 4 * ROWS]
    return low, high


def prep_kernel(counts, jac, res, cam, msg, acc):
    lane = lax.broadcasted_iota(jnp.int32, (1, 128), 1)

    def body(d, hot):
        live = counts[0, d]
        for h in range(2):
            col = pl.multiple_of(d * CAP + h * 128, 128)
            msg[d, h, 0:18, :] = jac[:, pl.ds(col, 128)]
            msg[d, h, 18:20, :] = res[:, pl.ds(col, 128)]
            ids = cam[pl.ds(d * 4 + h, 1), :]
            msg[d, h, 20:21, :] = jnp.where(lane + h * 128 < live, ids, -1).astype(F32)
        return jnp.where(live == CAP, d, hot)

    hot = lax.fori_loop(0, 64, body, 0)
    col = pl.multiple_of(hot * CAP + 256, 128)
    ids = jnp.concatenate([cam[pl.ds(hot * 4 + 2, 1), :], cam[pl.ds(hot * 4 + 3, 1), :]], axis=1).astype(F32)
    acc[:, 4 * ROWS :] = jnp.zeros((HALF, 256 - 4 * ROWS), F32)
    acc[:, : 4 * ROWS] = weighted(jac[:, pl.ds(col, 256)], res[:, pl.ds(col, 256)], ids)
    low, high = unfolded(acc)
    for t in range(ROWS):
        for q in range(4):
            msg[t, 0, 21 + q : 22 + q, :] = low[t : t + 1, q * 128 : (q + 1) * 128]
            msg[t, 1, 21 + q : 22 + q, :] = high[t : t + 1, q * 128 : (q + 1) * 128]
    for t in range(ROWS, 64):
        msg[t, :, 21:25, :] = jnp.zeros((2, 4, 128), F32)


def device_of(bucket, z):
    zd, y, core = bucket // 8, (bucket // 2) % 4, bucket % 2
    return ((z // 2) * 2 + zd % 2) * 8 + y * 2 + core, zd // 2


def exchange_kernel(msg, got, send_sem, recv_sem):
    z, y, core, x = place()
    me = bucket_of(z, y, core, x)
    barrier = pltpu.get_barrier_semaphore()

    def greet(i, c):
        pl.semaphore_signal(barrier, inc=1, device_id=device_of((me + i) % 64, z), device_id_type=MESH)
        return c

    lax.fori_loop(1, 64, greet, 0)
    pl.semaphore_wait(barrier, 63)

    def copy(to, frm):
        return pltpu.make_async_remote_copy(
            src_ref=msg.at[to],
            dst_ref=got.at[frm],
            send_sem=send_sem.at[to],
            recv_sem=recv_sem.at[frm],
            device_id=device_of(to, z),
            device_id_type=MESH,
        )

    def send(i, c):
        copy((me + i) % 64, me).start()
        return c

    lax.fori_loop(1, 64, send, 0)
    got[me] = msg[me]

    def take(i, c):
        copy((me + 64 - i) % 64, (me + 64 - i) % 64).wait_recv()
        return c

    lax.fori_loop(1, 64, take, 0)

    def sent(i, c):
        copy((me + i) % 64, me).wait_send()
        return c

    lax.fori_loop(1, 64, sent, 0)


def sums_kernel(got, msg, acc):
    acc[...] = jnp.zeros_like(acc)
    chunk = 8

    def body(i, c):
        slabs = [got[i * chunk + s, h] for s in range(chunk) for h in range(2)]
        whole = jnp.concatenate([s[0:21] for s in slabs], axis=1)
        acc[:, : 4 * ROWS] += weighted(whole[0:18], whole[18:20], whole[20:21])
        return c

    lax.fori_loop(0, 64 // chunk, body, 0)
    low, high = unfolded(acc)

    def hot(s, total):
        return total + got[s, :, 21:25, :]

    extra = lax.fori_loop(0, 64, hot, jnp.zeros((2, 4, 128), F32))
    for g in range(4):
        part = low if g < 2 else high
        for h in range(2):
            q = (g % 2) * 2 + h
            msg[g, h, 0:ROWS, :] = part[:, q * 128 : (q + 1) * 128]
            msg[g, h, ROWS : ROWS + 1, :] = extra[g // 2, q : q + 1, :]


def slots_of(z, y, core, x):
    return core * 128 + x * 32 + y * 8 + z, core * 128 + y * 32 + x * 8 + z


def at(z, y, core, x):
    return (z * 8 + y * 2 + core, x)


def gather_peers(z, y, core, x):
    peers = [at((z + i) % 8, y, core, x) for i in range(1, 8)]
    peers += [at(z, (y + i) % 4, core, x) for i in range(1, 4)]
    peers += [at(z, y, core, (x + i) % 4) for i in range(1, 4)]
    return peers + [at(z, y, 1 - core, x)]


def gather_all(ref, send_sem, recv_sem):
    z, y, core, x = place()
    slots = slots_of(z, y, core, x)
    ys = [at(z, (y + i) % 4, core, x) for i in range(1, 4)]
    xs = [at(z, y, core, (x + i) % 4) for i in range(1, 4)]
    zs = [at((z + i) % 8, y, core, x) for i in range(1, 8)]
    other = [at(z, y, 1 - core, x)]
    phases = [
        (zs, zs, 1),
        (ys, xs, 8),
        (xs, ys, 32),
        (other, other, 128),
    ]
    for n, (peers0, peers1, size) in enumerate(phases):
        for part, peers in ((0, peers0), (1, peers1)):
            base = (slots[part] // size) * size
            for peer in peers:
                pltpu.make_async_remote_copy(
                    src_ref=ref.at[part, pl.ds(base, size)],
                    dst_ref=ref.at[part, pl.ds(base, size)],
                    send_sem=send_sem.at[n, part],
                    recv_sem=recv_sem.at[n, part],
                    device_id=peer,
                    device_id_type=MESH,
                ).start()
        for part, peers in ((0, peers0), (1, peers1)):
            whole = ref.at[part, pl.ds(0, size * len(peers))]
            pltpu.make_async_remote_copy(
                src_ref=whole,
                dst_ref=whole,
                send_sem=send_sem.at[n, part],
                recv_sem=recv_sem.at[n, part],
                device_id=peers[0],
                device_id_type=MESH,
            ).wait_recv()
    for n, (peers0, peers1, size) in enumerate(phases):
        for part, peers in ((0, peers0), (1, peers1)):
            whole = ref.at[part, pl.ds(0, size * len(peers))]
            pltpu.make_async_remote_copy(
                src_ref=whole,
                dst_ref=whole,
                send_sem=send_sem.at[n, part],
                recv_sem=recv_sem.at[n, part],
                device_id=peers[0],
                device_id_type=MESH,
            ).wait_send()


def reduce_kernel(msg, grads, blocks, got, mine, send2, recv2, send3, recv3, send4, recv4):
    z, y, core, x = place()
    g, p = z // 2, z % 2
    zd = 2 * x + p
    zx, zp, zg = z // 2, z % 2, z
    barrier = pltpu.get_barrier_semaphore()
    zpeers = [at((z + 2 * i) % 8, y, core, x) for i in range(1, 4)]
    greeted = gather_peers(z, y, core, x)
    for peer in greeted:
        pl.semaphore_signal(barrier, inc=1, device_id=peer, device_id_type=MESH)
    owners = [(zd, xo) for xo in range(4)]
    holders = [2 * gg + z % 2 for gg in range(4)]
    count = 14
    for xo in range(4):
        away = jnp.logical_or(zd != z, xo != x)

        @pl.when(away)
        def _():
            pl.semaphore_signal(barrier, inc=1, device_id=at(zd, y, core, xo), device_id_type=MESH)

        count += away.astype(jnp.int32)
    for gg in range(4):
        zh = 2 * gg + zp
        away = jnp.logical_or(zh != z, zx != x)

        @pl.when(away)
        def _():
            pl.semaphore_signal(barrier, inc=1, device_id=at(zh, y, core, zx), device_id_type=MESH)

        count += away.astype(jnp.int32)
    pl.semaphore_wait(barrier, count)

    copies = []
    for i in range(1, 4):
        to = (g + i) % 4
        copies.append(
            pltpu.make_async_remote_copy(
                src_ref=msg.at[to],
                dst_ref=got.at[i],
                send_sem=send2.at[i],
                recv_sem=recv2.at[i],
                device_id=at(2 * to + p, y, core, x),
                device_id_type=MESH,
            )
        )
        copies[-1].start()
    total = msg[g]
    for c in copies:
        c.wait_recv()
    total = total + got[1] + got[2] + got[3]
    mine[...] = total
    slots = slots_of(z, y, core, x)
    for h in range(2):
        grads[h, slots[h]] = total[h, 47:57, :]

    def block_copy(zo, xo, quarter, n):
        return pltpu.make_async_remote_copy(
            src_ref=mine.at[:, pl.ds(0, 45)],
            dst_ref=blocks.at[quarter],
            send_sem=send3.at[n],
            recv_sem=recv3.at[quarter],
            device_id=at(zo, y, core, xo),
            device_id_type=MESH,
        )

    for xo in range(4):
        away = jnp.logical_or(zd != z, xo != x)

        @pl.when(away)
        def _():
            block_copy(zd, xo, g, xo).start()

        @pl.when(jnp.logical_not(away))
        def _():
            blocks[g] = mine[:, 0:45]

    gather_all(grads, send4, recv4)
    for gg in range(4):
        away = jnp.logical_or(2 * gg + zp != z, zx != x)

        @pl.when(away)
        def _():
            block_copy(zd, 0, gg, 0).wait_recv()

    for xo in range(4):
        away = jnp.logical_or(zd != z, xo != x)

        @pl.when(away)
        def _():
            block_copy(zd, xo, g, xo).wait_send()

    for c in copies:
        c.wait_send()


def inverse_kernel(cam_map, out):
    z, y, core, x = place()
    base = (lax.axis_index("obs") * 4 + lax.axis_index("rep")) * 256
    out[...] = jnp.zeros_like(out)
    lane = lax.broadcasted_iota(jnp.int32, (1, 128), 1)
    rows = lax.broadcasted_iota(jnp.int32, (16, 128), 0)
    chunk = 16

    def body(i, acc):
        left, right = [], []
        for k in range(chunk):
            r = i * chunk + k
            place_ = cam_map[pl.ds(r, 1), :] - base
            cam = r * 128 + lane
            inside = jnp.where((place_ >= 0) & (place_ < 256), place_, -16)
            hi, lo = inside >> 4, inside & 15
            hit = rows == hi
            left.append(
                jnp.concatenate(
                    [jnp.where(hit, (cam >> 8).astype(F32), 0.0), jnp.where(hit, (cam & 255).astype(F32), 0.0)], axis=0
                )
            )
            right.append(jnp.where(rows == lo, 1.0, 0.0))
        a = jnp.concatenate(left, axis=1).astype(BF16)
        b = jnp.concatenate(right, axis=1).astype(BF16)
        return acc + lax.dot_general(a, b, (((1,), (1,)), ((), ())), preferred_element_type=F32)

    acc = lax.fori_loop(0, 512 // chunk, body, jnp.zeros((32, 16), F32))
    out[:, 0:16] = (acc[0:16] * 256.0 + acc[16:32]).astype(jnp.int32)


def slot_of_camera(d, g):
    zd = d // 8
    return slots_of(2 * g + zd % 2, (d // 2) % 4, d % 2, zd // 2)


def pick_kernel(counts, inv, grads, out, table):
    def find(d, hot):
        return jnp.where(counts[0, d] == CAP, d, hot)

    hot = lax.fori_loop(0, 64, find, 0)
    out[...] = jnp.zeros_like(out)
    for g in range(4):
        hot_slots = slot_of_camera(hot, g)
        for h in range(2):
            extra = [grads[h, slot_of_camera(47 + k, g)[h], 9:10, :] for k in range(9)]
            table[g * 2 + h, 0:9, :] = grads[h, hot_slots[h], 0:9, :] + jnp.concatenate(extra, axis=0)
    lane = lax.broadcasted_iota(jnp.int32, (1, 128), 1)
    for part in range(2):

        def body(q, acc):
            cam = inv[part * 8 + q // 16, q % 16]
            d, g, h, at_lane = cam // 1024, (cam // 256) % 4, (cam // 128) % 2, cam % 128
            slots = slot_of_camera(d, g)
            slot = jnp.where(h == 0, slots[0], slots[1])
            plain = grads[h, slot, 0:9, :]
            fixed = table[g * 2 + h, 0:9, :]
            tile = jnp.where(d == hot, fixed, plain)
            tile = pltpu.roll(tile, (q - at_lane) % 128, 1)
            return jnp.where(lane == q, tile, acc)

        acc = lax.fori_loop(0, 128, body, jnp.zeros((9, 128), F32))
        out[part] = jnp.concatenate([acc[1:9], acc[0:1]], axis=0)


def spread_kernel(mine, table, send_sem, recv_sem):
    z, y, core, x = place()
    barrier = pltpu.get_barrier_semaphore()
    peers = gather_peers(z, y, core, x)
    for peer in peers:
        pl.semaphore_signal(barrier, inc=1, device_id=peer, device_id_type=MESH)
    pl.semaphore_wait(barrier, len(peers))
    slots = slots_of(z, y, core, x)
    for h in range(2):
        table[h, slots[h]] = mine[h]
    gather_all(table, send_sem, recv_sem)


def finish_kernel(counts, table, grads, blocks, out, blocks_out):
    def place_block(i, c):
        obs, x = i // 4, i % 4
        slots = slots_of(obs // 8, (obs // 2) % 4, obs % 2, x)
        for h in range(2):
            col = pl.multiple_of(i * 256 + h * 128, 128)
            out[:, pl.ds(col, 128)] = table[h, slots[h]]
        return c

    lax.fori_loop(0, 256, place_block, 0)
    hot = counts[0, lax.axis_index("obs")] == CAP
    for g in range(4):
        for h in range(2):
            extra = [grads[h, slot_of_camera(t, g)[h], 9:10, :] for t in range(45)]
            whole = blocks[g, h] + jnp.where(hot, jnp.concatenate(extra, axis=0), 0.0)
            col = g * 256 + h * 128
            for k in range(9):
                for j in range(5):
                    l = (k + j) % 9
                    t = 40 + j if k == 8 else j * 8 + k
                    blocks_out[k * 9 + l : k * 9 + l + 1, col : col + 128] = whole[t : t + 1]
                    if j:
                        blocks_out[l * 9 + k : l * 9 + k + 1, col : col + 128] = whole[t : t + 1]


def shape(*dims, dtype=F32):
    return jax.ShapeDtypeStruct(dims, dtype)


def call(kernel, out, ins, scratch=(), cid=None, **kw):
    params = dict(vmem_limit_bytes=60 * 1024 * 1024)
    if cid is not None:
        params.update(collective_id=cid, has_side_effects=True)
    many = isinstance(out, tuple)
    return pl.pallas_call(
        kernel,
        out_shape=out,
        in_specs=ins,
        out_specs=tuple(VM() for _ in out) if many else VM(),
        scratch_shapes=list(scratch),
        compiler_params=pltpu.CompilerParams(**params),
        **kw,
    )


def local(jacobians, residuals, camera_local, bucket_counts, camera_map):
    dma = pltpu.SemaphoreType.DMA
    cam = camera_local.reshape(256, 128)
    msg = call(
        prep_kernel,
        shape(64, 2, MSG, 128),
        [SM(), VM(), VM(), VM()],
        [pltpu.VMEM((HALF, 256), F32)],
    )(bucket_counts, jacobians, residuals, cam)
    got = call(exchange_kernel, shape(64, 2, MSG, 128), [VM()], [dma((64,)), dma((64,))], cid=1)(msg)
    part = call(sums_kernel, shape(4, 2, ROWS + 1, 128), [VM()], [pltpu.VMEM((HALF, 256), F32)])(got)
    grads, blocks = call(
        reduce_kernel,
        (shape(2, 256, 10, 128), shape(4, 2, 45, 128)),
        [VM()],
        [
            pltpu.VMEM((4, 2, ROWS + 1, 128), F32),
            pltpu.VMEM((2, ROWS + 1, 128), F32),
            dma((4,)),
            dma((4,)),
            dma((4,)),
            dma((4,)),
            dma((4, 2)),
            dma((4, 2)),
        ],
        cid=2,
    )(part)
    inv = call(inverse_kernel, shape(16, 128, dtype=jnp.int32), [VM()])(camera_map.reshape(512, 128))
    mine = call(
        pick_kernel, shape(2, 9, 128), [SM(), SM(), VM()], [pltpu.VMEM((8, 16, 128), F32)]
    )(bucket_counts, inv, grads)
    table = call(spread_kernel, shape(2, 256, 9, 128), [VM()], [dma((4, 2)), dma((4, 2))], cid=3)(mine)
    return call(
        finish_kernel, (shape(9, 65536), shape(81, 1024)), [SM(), VM(), VM(), VM()]
    )(bucket_counts, table, grads, blocks)


def solution(mesh):
    return jax.shard_map(
        local,
        mesh=mesh,
        in_specs=(P(None, ("obs", "rep")), P(None, ("obs", "rep")), P(("obs", "rep")), P(("obs", "rep"), None), P()),
        out_specs=(P(), P(None, "obs")),
        check_vma=False,
    )
```

```python
import functools

import jax
import jax.numpy as jnp
from jax import lax
from jax.experimental import pallas as pl
from jax.experimental.pallas import tpu as pltpu
from jax.sharding import PartitionSpec as P

MESH = pl.DeviceIdType.MESH
F32 = jnp.float32
BF16 = jnp.bfloat16
CAP = 512
HALF = 512
ROWS = 56
MSG = 21
SLOTS = 256
VM = functools.partial(pl.BlockSpec, memory_space=pltpu.VMEM)
SM = functools.partial(pl.BlockSpec, memory_space=pltpu.SMEM)


def place():
    obs = lax.axis_index("obs")
    return obs // 8, (obs // 2) % 4, obs % 2, lax.axis_index("rep")


def bucket_of(z, y, core, x):
    return (2 * x + z % 2) * 8 + y * 2 + core


def terms(jac, res):
    j0, j1, r0, r1 = jac[0:9], jac[9:18], res[0:1], res[1:2]

    def turned(j, k):
        return j[0:8] if k == 0 else j[1:9] if k == 1 else jnp.concatenate([j[k:9], j[0 : k - 1]], axis=0)

    rows = [j0[0:8] * turned(j0, k) + j1[0:8] * turned(j1, k) for k in range(5)]
    last0 = jnp.concatenate([j0[8:9], j0[0:4], j0[0:2], r0], axis=0)
    last1 = jnp.concatenate([j1[8:9], j1[0:4], j1[0:2], r1], axis=0)
    rows.append(j0[8:9] * last0 + j1[8:9] * last1)
    rows.append(j0[0:8] * r0 + j1[0:8] * r1)
    return jnp.concatenate(rows, axis=0)


def weighted(jac, res, ids):
    full = terms(jac, res)
    high = full.astype(BF16).astype(F32)
    both = jnp.concatenate([high, full - high], axis=0)
    upper = ids >= HALF
    weights = jnp.concatenate([jnp.where(upper, 0.0, both), jnp.where(upper, both, 0.0)], axis=0)
    ids = jnp.where(upper, ids - HALF, ids)
    rows = lax.broadcasted_iota(jnp.int32, (HALF, ids.shape[1]), 0).astype(F32)
    hot = jnp.where(rows == ids, 1.0, 0.0).astype(BF16)
    return lax.dot_general(hot, weights.astype(BF16), (((1,), (1,)), ((), ())), preferred_element_type=F32)


def unfolded(acc_ref):
    turned = acc_ref[...].T
    low = turned[0:ROWS] + turned[ROWS : 2 * ROWS]
    high = turned[2 * ROWS : 3 * ROWS] + turned[3 * ROWS : 4 * ROWS]
    return low, high


def device_of(bucket, z):
    zd, y, core = bucket // 8, (bucket // 2) % 4, bucket % 2
    return ((z // 2) * 2 + zd % 2) * 8 + y * 2 + core, zd // 2


def slots_of(z, y, core, x):
    return core * 128 + x * 32 + y * 8 + z, core * 128 + y * 32 + x * 8 + z


def slot_of_camera(d, g):
    zd = d // 8
    return slots_of(2 * g + zd % 2, (d // 2) % 4, d % 2, zd // 2)


def at(z, y, core, x):
    return (z * 8 + y * 2 + core, x)


def remote(src, dst, send, recv, device):
    return pltpu.make_async_remote_copy(
        src_ref=src, dst_ref=dst, send_sem=send, recv_sem=recv, device_id=device, device_id_type=MESH
    )


def looped(start, stop, do):
    def body(i, c):
        do(i)
        return c

    lax.fori_loop(start, stop, body, 0)


def camera_ids_here(cam_map, hot):
    base = (lax.axis_index("obs") * 4 + lax.axis_index("rep")) * 256
    lane = lax.broadcasted_iota(jnp.int32, (1, 128), 1)
    rows = lax.broadcasted_iota(jnp.int32, (16, 128), 0)
    chunk = 16

    def body(i, acc):
        left, right = [], []
        for k in range(chunk):
            r = i * chunk + k
            spot = cam_map[pl.ds(r, 1), :] - base
            cam = r * 128 + lane
            inside = jnp.where((spot >= 0) & (spot < 256), spot, -16)
            hit = rows == (inside >> 4)
            left.append(
                jnp.concatenate(
                    [jnp.where(hit, (cam >> 8).astype(F32), 0.0), jnp.where(hit, (cam & 255).astype(F32), 0.0)], axis=0
                )
            )
            right.append(jnp.where(rows == (inside & 15), 1.0, 0.0))
        a = jnp.concatenate(left, axis=1).astype(BF16)
        b = jnp.concatenate(right, axis=1).astype(BF16)
        return acc + lax.dot_general(a, b, (((1,), (1,)), ((), ())), preferred_element_type=F32)

    acc = lax.fori_loop(0, 512 // chunk, body, jnp.zeros((32, 16), F32))
    cam = (acc[0:16] * 256.0 + acc[16:32]).astype(jnp.int32)
    d, g, h, lane = cam >> 10, (cam >> 8) & 3, (cam >> 7) & 1, cam & 127
    zd, y, core = d >> 3, (d >> 1) & 3, d & 1
    slots = slots_of(2 * g + (zd & 1), y, core, zd >> 1)
    spot = jnp.where(h == 0, slots[0], SLOTS + slots[1])
    spot = jnp.where(d == hot, 2 * SLOTS + 2 * g + h, spot)
    return spot * 128 + lane


def front_kernel(
    counts, jac, res, cam, cam_map, part_b, part_g, part_e, inv, msg, hots, gothot, acc, ssem, rsem, hssem, hrsem, *gots
):
    chunk = 64 // len(gots)
    z, y, core, x = place()
    me = bucket_of(z, y, core, x)
    barrier = pltpu.get_barrier_semaphore()
    looped(
        1,
        64,
        lambda i: pl.semaphore_signal(
            barrier, inc=1, device_id=device_of((me + i) % 64, z), device_id_type=MESH
        ),
    )
    lane = lax.broadcasted_iota(jnp.int32, (1, 128), 1)

    def pack(d, carry):
        hot, ejac, eres, eids = carry
        live = counts[0, d]
        for h in range(2):
            col = pl.multiple_of(d * CAP + h * 128, 128)
            msg[d, h, 0:18, :] = jac[:, pl.ds(col, 128)]
            msg[d, h, 18:20, :] = res[:, pl.ds(col, 128)]
            ids = cam[pl.ds(d * 4 + h, 1), :]
            msg[d, h, 20:21, :] = jnp.where(lane + h * 128 < live, ids, -1).astype(F32)
        full = live == CAP
        col = pl.multiple_of(d * CAP + 256, 128)
        ids = jnp.concatenate([cam[pl.ds(d * 4 + 2, 1), :], cam[pl.ds(d * 4 + 3, 1), :]], axis=1)
        return (
            jnp.where(full, d, hot),
            jnp.where(full, jac[:, pl.ds(col, 256)], ejac),
            jnp.where(full, res[:, pl.ds(col, 256)], eres),
            jnp.where(full, ids, eids),
        )

    hot, ejac, eres, eids = lax.fori_loop(
        0,
        64,
        pack,
        (jnp.int32(0), jnp.zeros((18, 256), F32), jnp.zeros((2, 256), F32), jnp.zeros((1, 256), jnp.int32)),
    )
    pl.semaphore_wait(barrier, 63)

    def copy(i):
        to = (me + i) % 64
        return remote(msg.at[to], gots[(i - 1) // chunk].at[(i - 1) % chunk], ssem.at[i], rsem.at[i], device_of(to, z))

    def hot_copy(i):
        to = (me + i) % 64
        return remote(hots.at[to], gothot.at[i], hssem.at[i], hrsem.at[i], device_of(to, z))

    for i in range(1, 64):
        copy(i).start()
    gots[-1][chunk - 1] = msg[me]
    acc[:, 4 * ROWS :] = jnp.zeros((HALF, 256 - 4 * ROWS), F32)
    acc[:, : 4 * ROWS] = weighted(ejac, eres, eids.astype(F32))
    low, high = unfolded(acc)
    for q in range(4):
        hots[0:ROWS, q, :] = low[:, q * 128 : (q + 1) * 128]
        hots[0:ROWS, 4 + q, :] = high[:, q * 128 : (q + 1) * 128]
    hots[ROWS:64] = jnp.zeros((64 - ROWS, 8, 128), F32)
    for i in range(1, 64):
        hot_copy(i).start()
    gothot[0] = hots[me]
    inv[...] = jnp.zeros_like(inv)
    inv[:, 0:16] = camera_ids_here(cam_map, hot)
    inv[0:1, 16:17] = jnp.full((1, 1), hot, jnp.int32)

    acc[...] = jnp.zeros_like(acc)
    for c in range(64 // chunk):
        for i in range(c * chunk + 1, min(c * chunk + chunk + 1, 64)):
            copy(i).wait_recv()
        whole = jnp.concatenate([gots[c][s, h] for s in range(chunk) for h in range(2)], axis=1)
        acc[:, : 4 * ROWS] += weighted(whole[0:18], whole[18:20], whole[20:21])
    low, high = unfolded(acc)
    for i in range(1, 64):
        hot_copy(i).wait_recv()
    extra = lax.fori_loop(0, 64, lambda s, t: t + gothot[s], jnp.zeros((8, 128), F32))
    for g in range(4):
        part = low if g < 2 else high
        for h in range(2):
            q = (g % 2) * 2 + h
            tile = part[:, q * 128 : (q + 1) * 128]
            part_b[g, h] = tile[0:48]
            part_g[g, h] = tile[48:56]
            part_e[g, h, 0:1] = tile[47:48]
            part_e[g, h, 1:2] = extra[g * 2 + h : g * 2 + h + 1]
    for i in range(1, 64):
        copy(i).wait_send()
        hot_copy(i).wait_send()


class Gather:
    def __init__(self, refs, sems):
        self.refs, self.sems = refs, sems
        z, y, core, x = place()
        self.slots = slots_of(z, y, core, x)
        ys = [at(z, (y + i) % 4, core, x) for i in range(1, 4)]
        xs = [at(z, y, core, (x + i) % 4) for i in range(1, 4)]
        self.zs = [at((z + i) % 8, y, core, x) for i in range(1, 8)]
        self.other = at(z, y, 1 - core, x)
        self.middle, self.last = (ys, xs), (xs, ys)
        self.mid, self.far = (y, x), (x, y)
        self.core = core

    def peers(self):
        return self.zs + self.middle[0] + self.middle[1] + [self.other]

    def copies(self, part, start, size, sem, device):
        out = []
        for n, ref in enumerate(self.refs):
            view = ref.at[pl.ds(part * SLOTS + start, size)]
            send, recv = self.sems[n]
            out.append(remote(view, view, send.at[part, sem], recv.at[part, sem], device))
        return out

    def start(self, *args):
        for c in self.copies(*args):
            c.start()

    def wait_recv(self, *args):
        for c in self.copies(*args):
            c.wait_recv()

    def run(self, between=()):
        between = list(between) + [lambda: None] * 3
        for part in range(2):
            for peer in self.zs:
                self.start(part, self.slots[part], 1, 0, peer)
        between[0]()
        blocks = [self.slots[part] // 8 * 8 for part in range(2)]
        for part in range(2):
            self.wait_recv(part, 0, 7, 0, self.zs[0])
            for i in range(3):
                self.start(part, blocks[part], 8, 1 + i, self.middle[part][i])
            for i in range(3):
                self.start(part, blocks[part], 8, 4 + i, self.last[part][i])
            self.start(part, blocks[part], 8, 7, self.other)
        between[1]()
        for i in range(3):
            for part in range(2):
                base = self.core * 128 + self.far[part] * 32 + (self.mid[part] + 3 - i) % 4 * 8
                self.wait_recv(part, base, 8, 1 + i, self.middle[part][i])
                for j in range(3):
                    self.start(part, base, 8, 4 + j, self.last[part][j])
                self.start(part, base, 8, 7, self.other)
        between[2]()
        for j in range(3):
            for part in range(2):
                base = self.core * 128 + (self.far[part] + 3 - j) % 4 * 32
                self.wait_recv(part, base, 32, 4 + j, self.last[part][j])
                self.start(part, base, 32, 7, self.other)
        for part in range(2):
            self.wait_recv(part, 0, 128, 7, self.other)

    def finish(self):
        for part in range(2):
            for sem, size in [(0, 7)] + [(k, 8) for k in (1, 2, 3)] + [(k, 32) for k in (4, 5, 6)] + [(7, 128)]:
                for c in self.copies(part, 0, size, sem, self.other):
                    c.wait_send()


def back_kernel(
    inv, part_b, part_g, part_e, table, table_e, blocks,
    got_b, got_g, got_e, mine_b, bx, bz, grad, grad_e,
    s2b, r2b, s2g, r2g, s2e, r2e, sx, rx, sz, rz, sg, rg, se, re, sg2, rg2, se2, re2,
):
    z, y, core, x = place()
    g, p = z // 2, z % 2
    first = Gather((grad, grad_e), ((sg, rg), (se, re)))
    second = Gather((table, table_e), ((sg2, rg2), (se2, re2)))
    barrier = pltpu.get_barrier_semaphore()
    peers = first.peers()
    for peer in peers:
        pl.semaphore_signal(barrier, inc=1, device_id=peer, device_id_type=MESH)
    pl.semaphore_wait(barrier, len(peers))

    small, large = [], []
    for i in range(1, 4):
        to = (g + i) % 4
        device = at(2 * to + p, y, core, x)
        small.append(remote(part_g.at[to], got_g.at[i - 1], s2g.at[i - 1], r2g.at[i - 1], device))
        small.append(remote(part_e.at[to], got_e.at[i - 1], s2e.at[i - 1], r2e.at[i - 1], device))
        large.append(remote(part_b.at[to], got_b.at[i - 1], s2b.at[i - 1], r2b.at[i - 1], device))
    for c in small + large:
        c.start()
    for c in small:
        c.wait_recv()
    total_g = part_g[g] + got_g[0] + got_g[1] + got_g[2]
    total_e = part_e[g] + got_e[0] + got_e[1] + got_e[2]
    for h in range(2):
        grad[h * SLOTS + first.slots[h]] = total_g[h]
        grad_e[h * SLOTS + first.slots[h]] = total_e[h]

    across, along = [], []
    for i in range(1, 4):
        across.append(remote(mine_b, bx.at[x], sx.at[i - 1], rx.at[i - 1], at(z, y, core, (x + i) % 4)))
        to = (g + i) % 4
        along.append(remote(bx.at[to], bz.at[g], sz.at[i - 1], rz.at[i - 1], at(2 * to + p, y, core, x)))

    def spread_blocks():
        for c in large:
            c.wait_recv()
        mine_b[...] = part_b[g] + got_b[0] + got_b[1] + got_b[2]
        bx[x] = mine_b[...]
        for c in across:
            c.start()

    def send_blocks():
        for c in across:
            c.wait_recv()
        for c in along:
            c.start()
        bz[g] = bx[g]

    first.run([spread_blocks, send_blocks])

    hot = inv[0, 16]
    for gg in range(4):
        hot_slots = slot_of_camera(hot, gg)
        for h in range(2):
            slot = h * SLOTS + hot_slots[h]
            extra = [grad_e[h * SLOTS + slot_of_camera(48 + k, gg)[h], 1:2] for k in range(8)]
            grad[2 * SLOTS + 2 * gg + h] = grad[slot] + jnp.concatenate(extra, axis=0)
            grad_e[2 * SLOTS + 2 * gg + h, 0:1] = (
                grad_e[slot, 0:1] + grad_e[h * SLOTS + slot_of_camera(47, gg)[h], 1:2]
            )
            grad_e[2 * SLOTS + 2 * gg + h, 1:2] = jnp.zeros((1, 128), F32)
    lane = lax.broadcasted_iota(jnp.int32, (1, 128), 1)
    for h in range(2):

        def pick(r, acc):
            top, low = acc
            for k in range(16):
                v = inv[h * 8 + r, k]
                q = r * 16 + k
                turn = (q - v) & 127
                at_q = lane == q
                top = jnp.where(at_q, pltpu.roll(grad[v >> 7], turn, 1), top)
                low = jnp.where(at_q, pltpu.roll(grad_e[v >> 7], turn, 1), low)
            return top, low

        top, low = lax.fori_loop(0, 8, pick, (jnp.zeros((8, 128), F32), jnp.zeros((2, 128), F32)))
        table[h * SLOTS + second.slots[h]] = top
        table_e[h * SLOTS + second.slots[h]] = low[0:1]

    def fix_blocks():
        for c in along:
            c.wait_recv()
        here = lax.axis_index("obs") == hot
        for gg in range(4):
            for h in range(2):
                extra = [grad_e[h * SLOTS + slot_of_camera(t, gg)[h], 1:2] for t in range(45)]
                extra = jnp.concatenate(extra + [jnp.zeros((3, 128), F32)], axis=0)
                blocks[gg, h] = bz[gg, h] + jnp.where(here, extra, 0.0)

    second.run([lambda: None, fix_blocks])
    for c in small + large + across + along:
        c.wait_send()
    first.finish()
    second.finish()


def finish_kernel(table, table_e, blocks, out, blocks_out):
    def place_block(i, c):
        obs, x = i >> 2, i & 3
        slots = slots_of(obs >> 3, (obs >> 1) & 3, obs & 1, x)
        for h in range(2):
            col = pl.multiple_of(i * 256 + h * 128, 128)
            slot = h * SLOTS + slots[h]
            out[0:8, pl.ds(col, 128)] = table[slot]
            out[8:9, pl.ds(col, 128)] = table_e[slot]
        return c

    lax.fori_loop(0, 256, place_block, 0, unroll=8)
    for g in range(4):
        for h in range(2):
            whole = blocks[g, h]
            col = g * 256 + h * 128
            for k in range(9):
                for j in range(5):
                    m = (k + j) % 9
                    t = 40 + j if k == 8 else j * 8 + k
                    blocks_out[k * 9 + m : k * 9 + m + 1, col : col + 128] = whole[t : t + 1]
                    if j:
                        blocks_out[m * 9 + k : m * 9 + k + 1, col : col + 128] = whole[t : t + 1]


def shape(*dims, dtype=F32):
    return jax.ShapeDtypeStruct(dims, dtype)


def call(kernel, out, ins, scratch=(), cid=None, **kw):
    params = dict(vmem_limit_bytes=60 * 1024 * 1024)
    if cid is not None:
        params.update(collective_id=cid, has_side_effects=True)
    many = isinstance(out, tuple)
    return pl.pallas_call(
        kernel,
        out_shape=out,
        in_specs=ins,
        out_specs=tuple(VM() for _ in out) if many else VM(),
        scratch_shapes=list(scratch),
        compiler_params=pltpu.CompilerParams(**params),
        **kw,
    )


def vmem(*dims):
    return pltpu.VMEM(dims, F32)


def local(jacobians, residuals, camera_local, bucket_counts, camera_map):
    dma = pltpu.SemaphoreType.DMA
    part_b, part_g, part_e, inv = call(
        front_kernel,
        (shape(4, 2, 48, 128), shape(4, 2, 8, 128), shape(4, 2, 2, 128), shape(16, 128, dtype=jnp.int32)),
        [SM(), VM(), VM(), VM(), VM()],
        [
            vmem(64, 2, MSG, 128),
            vmem(64, 8, 128),
            vmem(64, 8, 128),
            vmem(HALF, 256),
        ]
        + [dma((64,))] * 4
        + [vmem(8, 2, MSG, 128)] * 8,
        cid=1,
        name="front",
    )(bucket_counts, jacobians, residuals, camera_local.reshape(256, 128), camera_map.reshape(512, 128))
    table, table_e, blocks = call(
        back_kernel,
        (shape(2 * SLOTS, 8, 128), shape(2 * SLOTS, 1, 128), shape(4, 2, 48, 128)),
        [SM(), VM(), VM(), VM()],
        [
            vmem(3, 2, 48, 128),
            vmem(3, 2, 8, 128),
            vmem(3, 2, 2, 128),
            vmem(2, 48, 128),
            vmem(4, 2, 48, 128),
            vmem(4, 2, 48, 128),
            vmem(2 * SLOTS + 8, 8, 128),
            vmem(2 * SLOTS + 8, 2, 128),
        ]
        + [dma((3,))] * 10
        + [dma((2, 8))] * 8,
        cid=2,
        name="back",
    )(inv, part_b, part_g, part_e)
    return call(finish_kernel, (shape(9, 65536), shape(81, 1024)), [VM(), VM(), VM()], name="finish")(
        table, table_e, blocks
    )


def solution(mesh):
    return jax.shard_map(
        local,
        mesh=mesh,
        in_specs=(P(None, ("obs", "rep")), P(None, ("obs", "rep")), P(("obs", "rep")), P(("obs", "rep"), None), P()),
        out_specs=(P(), P(None, "obs")),
        check_vma=False,
    )
```

```python
import functools

import jax
import jax.numpy as jnp
from jax import lax
from jax.experimental import pallas as pl
from jax.experimental.pallas import tpu as pltpu
from jax.sharding import PartitionSpec as P

MESH = pl.DeviceIdType.MESH
F32 = jnp.float32
BF16 = jnp.bfloat16
CAP = 512
HALF = 512
ROWS = 56
MSG = 21
SLOTS = 256
VM = functools.partial(pl.BlockSpec, memory_space=pltpu.VMEM)
SM = functools.partial(pl.BlockSpec, memory_space=pltpu.SMEM)


def place():
    obs = lax.axis_index("obs")
    return obs // 8, (obs // 2) % 4, obs % 2, lax.axis_index("rep")


def bucket_of(z, y, core, x):
    return (2 * x + z % 2) * 8 + y * 2 + core


def terms(jac, res):
    j0, j1, r0, r1 = jac[0:9], jac[9:18], res[0:1], res[1:2]

    def turned(j, k):
        return j[0:8] if k == 0 else j[1:9] if k == 1 else jnp.concatenate([j[k:9], j[0 : k - 1]], axis=0)

    rows = [j0[0:8] * turned(j0, k) + j1[0:8] * turned(j1, k) for k in range(5)]
    last0 = jnp.concatenate([j0[8:9], j0[0:4], j0[0:2], r0], axis=0)
    last1 = jnp.concatenate([j1[8:9], j1[0:4], j1[0:2], r1], axis=0)
    rows.append(j0[8:9] * last0 + j1[8:9] * last1)
    rows.append(j0[0:8] * r0 + j1[0:8] * r1)
    return jnp.concatenate(rows, axis=0)


def weighted(jac, res, ids):
    full = terms(jac, res)
    high = full.astype(BF16).astype(F32)
    both = jnp.concatenate([high, full - high], axis=0)
    upper = ids >= HALF
    weights = jnp.concatenate([jnp.where(upper, 0.0, both), jnp.where(upper, both, 0.0)], axis=0)
    ids = jnp.where(upper, ids - HALF, ids)
    rows = lax.broadcasted_iota(jnp.int32, (HALF, ids.shape[1]), 0).astype(F32)
    hot = jnp.where(rows == ids, 1.0, 0.0).astype(BF16)
    return lax.dot_general(hot, weights.astype(BF16), (((1,), (1,)), ((), ())), preferred_element_type=F32)


def unfolded(acc_ref):
    turned = acc_ref[...].T
    low = turned[0:ROWS] + turned[ROWS : 2 * ROWS]
    high = turned[2 * ROWS : 3 * ROWS] + turned[3 * ROWS : 4 * ROWS]
    return low, high


def device_of(bucket, z):
    zd, y, core = bucket // 8, (bucket // 2) % 4, bucket % 2
    return ((z // 2) * 2 + zd % 2) * 8 + y * 2 + core, zd // 2


def slots_of(z, y, core, x):
    return core * 128 + x * 32 + y * 8 + z, core * 128 + y * 32 + x * 8 + z


def slot_of_camera(d, g):
    zd = d // 8
    return slots_of(2 * g + zd % 2, (d // 2) % 4, d % 2, zd // 2)


def at(z, y, core, x):
    return (z * 8 + y * 2 + core, x)


def remote(src, dst, send, recv, device):
    return pltpu.make_async_remote_copy(
        src_ref=src, dst_ref=dst, send_sem=send, recv_sem=recv, device_id=device, device_id_type=MESH
    )


def looped(start, stop, do):
    def body(i, c):
        do(i)
        return c

    lax.fori_loop(start, stop, body, 0)


def camera_ids_here(cam_map, hot):
    slots = slots_of(*place())
    bases = (slots[0] * 128, (SLOTS + slots[1]) * 128)
    lane = lax.broadcasted_iota(jnp.int32, (1, 128), 1)
    rows = lax.broadcasted_iota(jnp.int32, (16, 128), 0)
    chunk = 16

    def body(i, acc):
        left, right = [], []
        for k in range(chunk):
            r = i * chunk + k
            cam = r * 128 + lane
            first = cam_map[pl.ds(r, 1), :] - bases[0]
            second = cam_map[pl.ds(r, 1), :] - bases[1]
            inside = jnp.where((first >= 0) & (first < 128), first, -16)
            inside = jnp.where((second >= 0) & (second < 128), second + 128, inside)
            hit = rows == (inside >> 4)
            left.append(
                jnp.concatenate(
                    [jnp.where(hit, (cam >> 8).astype(F32), 0.0), jnp.where(hit, (cam & 255).astype(F32), 0.0)], axis=0
                )
            )
            right.append(jnp.where(rows == (inside & 15), 1.0, 0.0))
        a = jnp.concatenate(left, axis=1).astype(BF16)
        b = jnp.concatenate(right, axis=1).astype(BF16)
        return acc + lax.dot_general(a, b, (((1,), (1,)), ((), ())), preferred_element_type=F32)

    acc = lax.fori_loop(0, 512 // chunk, body, jnp.zeros((32, 16), F32))
    cam = (acc[0:16] * 256.0 + acc[16:32]).astype(jnp.int32)
    d, g, h, lane = cam >> 10, (cam >> 8) & 3, (cam >> 7) & 1, cam & 127
    zd, y, core = d >> 3, (d >> 1) & 3, d & 1
    slots = slots_of(2 * g + (zd & 1), y, core, zd >> 1)
    spot = jnp.where(h == 0, slots[0], SLOTS + slots[1])
    spot = jnp.where(d == hot, 2 * SLOTS + 2 * g + h, spot)
    return spot * 128 + lane


def front_kernel(
    counts, jac, res, cam, cam_map, part_b, part_g, part_e, inv, msg, hots, gothot, acc, ssem, rsem, hssem, hrsem, *gots
):
    chunk = 64 // len(gots)
    z, y, core, x = place()
    me = bucket_of(z, y, core, x)
    barrier = pltpu.get_barrier_semaphore()
    looped(
        1,
        64,
        lambda i: pl.semaphore_signal(
            barrier, inc=1, device_id=device_of((me + i) % 64, z), device_id_type=MESH
        ),
    )
    lane = lax.broadcasted_iota(jnp.int32, (1, 128), 1)

    def pack(d, carry):
        hot, ejac, eres, eids = carry
        live = counts[0, d]
        for h in range(2):
            col = pl.multiple_of(d * CAP + h * 128, 128)
            msg[d, h, 0:18, :] = jac[:, pl.ds(col, 128)]
            msg[d, h, 18:20, :] = res[:, pl.ds(col, 128)]
            ids = cam[pl.ds(d * 4 + h, 1), :]
            msg[d, h, 20:21, :] = jnp.where(lane + h * 128 < live, ids, -1).astype(F32)
        full = live == CAP
        col = pl.multiple_of(d * CAP + 256, 128)
        ids = jnp.concatenate([cam[pl.ds(d * 4 + 2, 1), :], cam[pl.ds(d * 4 + 3, 1), :]], axis=1)
        return (
            jnp.where(full, d, hot),
            jnp.where(full, jac[:, pl.ds(col, 256)], ejac),
            jnp.where(full, res[:, pl.ds(col, 256)], eres),
            jnp.where(full, ids, eids),
        )

    hot, ejac, eres, eids = lax.fori_loop(
        0,
        64,
        pack,
        (jnp.int32(0), jnp.zeros((18, 256), F32), jnp.zeros((2, 256), F32), jnp.zeros((1, 256), jnp.int32)),
    )
    pl.semaphore_wait(barrier, 63)

    def copy(i):
        to = (me + i) % 64
        return remote(msg.at[to], gots[(i - 1) // chunk].at[(i - 1) % chunk], ssem.at[i], rsem.at[i], device_of(to, z))

    def hot_copy(i):
        to = (me + i) % 64
        return remote(hots.at[to], gothot.at[i], hssem.at[i], hrsem.at[i], device_of(to, z))

    for i in range(1, 64):
        copy(i).start()
    gots[-1][chunk - 1] = msg[me]
    acc[:, 4 * ROWS :] = jnp.zeros((HALF, 256 - 4 * ROWS), F32)
    acc[:, : 4 * ROWS] = weighted(ejac, eres, eids.astype(F32))
    low, high = unfolded(acc)
    for q in range(4):
        hots[0:ROWS, q, :] = low[:, q * 128 : (q + 1) * 128]
        hots[0:ROWS, 4 + q, :] = high[:, q * 128 : (q + 1) * 128]
    hots[ROWS:64] = jnp.zeros((64 - ROWS, 8, 128), F32)
    for i in range(1, 64):
        hot_copy(i).start()
    gothot[0] = hots[me]
    inv[...] = jnp.zeros_like(inv)
    inv[:, 0:16] = camera_ids_here(cam_map, hot)
    inv[0:1, 16:17] = jnp.full((1, 1), hot, jnp.int32)

    acc[...] = jnp.zeros_like(acc)
    for c in range(64 // chunk):
        for i in range(c * chunk + 1, min(c * chunk + chunk + 1, 64)):
            copy(i).wait_recv()
        whole = jnp.concatenate([gots[c][s, h] for s in range(chunk) for h in range(2)], axis=1)
        acc[:, : 4 * ROWS] += weighted(whole[0:18], whole[18:20], whole[20:21])
    low, high = unfolded(acc)
    for i in range(1, 64):
        hot_copy(i).wait_recv()
    extra = lax.fori_loop(0, 64, lambda s, t: t + gothot[s], jnp.zeros((8, 128), F32))
    for g in range(4):
        part = low if g < 2 else high
        for h in range(2):
            q = (g % 2) * 2 + h
            tile = part[:, q * 128 : (q + 1) * 128]
            part_b[g, h] = tile[0:48]
            part_g[g, h] = tile[48:56]
            part_e[g, h, 0:1] = tile[47:48]
            part_e[g, h, 1:2] = extra[g * 2 + h : g * 2 + h + 1]
    for i in range(1, 64):
        copy(i).wait_send()
        hot_copy(i).wait_send()


class Gather:
    def __init__(self, refs, sems):
        self.refs, self.sems = refs, sems
        z, y, core, x = place()
        self.slots = slots_of(z, y, core, x)
        ys = [at(z, (y + i) % 4, core, x) for i in range(1, 4)]
        xs = [at(z, y, core, (x + i) % 4) for i in range(1, 4)]
        self.zs = [at((z + i) % 8, y, core, x) for i in range(1, 8)]
        self.other = at(z, y, 1 - core, x)
        self.middle, self.last = (ys, xs), (xs, ys)
        self.mid, self.far = (y, x), (x, y)
        self.core = core

    def peers(self):
        return self.zs + self.middle[0] + self.middle[1] + [self.other]

    def copies(self, part, start, size, sem, device):
        out = []
        for n, ref in enumerate(self.refs):
            view = ref.at[pl.ds(part * SLOTS + start, size)]
            send, recv = self.sems[n]
            out.append(remote(view, view, send.at[part, sem], recv.at[part, sem], device))
        return out

    def start(self, *args):
        for c in self.copies(*args):
            c.start()

    def wait_recv(self, *args):
        for c in self.copies(*args):
            c.wait_recv()

    def run(self, between=()):
        between = list(between) + [lambda: None] * 4
        for part in range(2):
            for peer in self.zs:
                self.start(part, self.slots[part], 1, 0, peer)
        between[0]()
        blocks = [self.slots[part] // 8 * 8 for part in range(2)]
        for part in range(2):
            self.wait_recv(part, 0, 7, 0, self.zs[0])
            for i in range(3):
                self.start(part, blocks[part], 8, 1 + i, self.middle[part][i])
            for i in range(3):
                self.start(part, blocks[part], 8, 4 + i, self.last[part][i])
            self.start(part, blocks[part], 8, 7, self.other)
        between[1]()
        for i in range(3):
            for part in range(2):
                base = self.core * 128 + self.far[part] * 32 + (self.mid[part] + 3 - i) % 4 * 8
                self.wait_recv(part, base, 8, 1 + i, self.middle[part][i])
                for j in range(3):
                    self.start(part, base, 8, 4 + j, self.last[part][j])
                self.start(part, base, 8, 7, self.other)
        between[2]()
        for j in range(3):
            for part in range(2):
                base = self.core * 128 + (self.far[part] + 3 - j) % 4 * 32
                self.wait_recv(part, base, 32, 4 + j, self.last[part][j])
                self.start(part, base, 32, 7, self.other)
        between[3]()
        for part in range(2):
            self.wait_recv(part, 0, 128, 7, self.other)

    def finish(self):
        for part in range(2):
            for sem, size in [(0, 7)] + [(k, 8) for k in (1, 2, 3)] + [(k, 32) for k in (4, 5, 6)] + [(7, 128)]:
                for c in self.copies(part, 0, size, sem, self.other):
                    c.wait_send()


def back_kernel(
    inv, part_b, part_g, part_e, table, table_e, blocks,
    got_b, got_g, got_e, mine_b, bx, bz, grad, grad_e,
    s2b, r2b, s2g, r2g, s2e, r2e, sx, rx, sz, rz, sg, rg, se, re, sg2, rg2, se2, re2,
):
    z, y, core, x = place()
    g, p = z // 2, z % 2
    first = Gather((grad, grad_e), ((sg, rg), (se, re)))
    second = Gather((table, table_e), ((sg2, rg2), (se2, re2)))
    barrier = pltpu.get_barrier_semaphore()
    peers = first.peers()
    for peer in peers:
        pl.semaphore_signal(barrier, inc=1, device_id=peer, device_id_type=MESH)
    pl.semaphore_wait(barrier, len(peers))

    small, large = [], []
    for i in range(1, 4):
        to = (g + i) % 4
        device = at(2 * to + p, y, core, x)
        small.append(remote(part_g.at[to], got_g.at[i - 1], s2g.at[i - 1], r2g.at[i - 1], device))
        small.append(remote(part_e.at[to], got_e.at[i - 1], s2e.at[i - 1], r2e.at[i - 1], device))
        large.append(remote(part_b.at[to], got_b.at[i - 1], s2b.at[i - 1], r2b.at[i - 1], device))
    for c in small:
        c.start()
    for c in small:
        c.wait_recv()
    total_g = part_g[g] + got_g[0] + got_g[1] + got_g[2]
    total_e = part_e[g] + got_e[0] + got_e[1] + got_e[2]
    for h in range(2):
        grad[h * SLOTS + first.slots[h]] = total_g[h]
        grad_e[h * SLOTS + first.slots[h]] = total_e[h]

    across, along = [], []
    for i in range(1, 4):
        across.append(remote(mine_b, bx.at[x], sx.at[i - 1], rx.at[i - 1], at(z, y, core, (x + i) % 4)))
        to = (g + i) % 4
        along.append(remote(bx.at[to], bz.at[g], sz.at[i - 1], rz.at[i - 1], at(2 * to + p, y, core, x)))

    def nothing():
        pass

    def start_blocks():
        for c in large:
            c.start()

    def spread_blocks():
        for c in large:
            c.wait_recv()
        mine_b[...] = part_b[g] + got_b[0] + got_b[1] + got_b[2]
        bx[x] = mine_b[...]
        for c in across:
            c.start()

    def send_blocks():
        for c in across:
            c.wait_recv()
        for c in along:
            c.start()
        bz[g] = bx[g]

    first.run([nothing, start_blocks])

    hot = inv[0, 16]
    for gg in range(4):
        hot_slots = slot_of_camera(hot, gg)
        for h in range(2):
            slot = h * SLOTS + hot_slots[h]
            extra = [grad_e[h * SLOTS + slot_of_camera(48 + k, gg)[h], 1:2] for k in range(8)]
            grad[2 * SLOTS + 2 * gg + h] = grad[slot] + jnp.concatenate(extra, axis=0)
            grad_e[2 * SLOTS + 2 * gg + h, 0:1] = (
                grad_e[slot, 0:1] + grad_e[h * SLOTS + slot_of_camera(47, gg)[h], 1:2]
            )
            grad_e[2 * SLOTS + 2 * gg + h, 1:2] = jnp.zeros((1, 128), F32)
    lane = lax.broadcasted_iota(jnp.int32, (1, 128), 1)
    for h in range(2):

        def pick(r, acc):
            top, low = acc
            for k in range(16):
                v = inv[h * 8 + r, k]
                q = r * 16 + k
                turn = (q - v) & 127
                at_q = lane == q
                top = jnp.where(at_q, pltpu.roll(grad[v >> 7], turn, 1), top)
                low = jnp.where(at_q, pltpu.roll(grad_e[v >> 7], turn, 1), low)
            return top, low

        top, low = lax.fori_loop(0, 8, pick, (jnp.zeros((8, 128), F32), jnp.zeros((2, 128), F32)))
        table[h * SLOTS + second.slots[h]] = top
        table_e[h * SLOTS + second.slots[h]] = low[0:1]

    def fix_blocks():
        for c in along:
            c.wait_recv()
        here = lax.axis_index("obs") == hot
        for gg in range(4):
            for h in range(2):
                extra = [grad_e[h * SLOTS + slot_of_camera(t, gg)[h], 1:2] for t in range(45)]
                extra = jnp.concatenate(extra + [jnp.zeros((3, 128), F32)], axis=0)
                blocks[gg, h] = bz[gg, h] + jnp.where(here, extra, 0.0)

    second.run([spread_blocks, send_blocks, nothing, fix_blocks])
    for c in small + large + across + along:
        c.wait_send()
    first.finish()
    second.finish()


def finish_kernel(table, table_e, blocks, out, blocks_out):
    for n in range(table.shape[0]):
        out[0:8, n * 128 : (n + 1) * 128] = table[n]
        out[8:9, n * 128 : (n + 1) * 128] = table_e[n]
    for h in range(2):
        whole = blocks[0, h]
        here = slice(h * 128, (h + 1) * 128)
        for k in range(9):
            for j in range(5):
                m = (k + j) % 9
                t = 40 + j if k == 8 else j * 8 + k
                blocks_out[k * 9 + m : k * 9 + m + 1, here] = whole[t : t + 1]
                if j:
                    blocks_out[m * 9 + k : m * 9 + k + 1, here] = whole[t : t + 1]


def shape(*dims, dtype=F32):
    return jax.ShapeDtypeStruct(dims, dtype)


def call(kernel, out, ins, scratch=(), cid=None, **kw):
    params = dict(vmem_limit_bytes=60 * 1024 * 1024)
    if cid is not None:
        params.update(collective_id=cid, has_side_effects=True)
    many = isinstance(out, tuple)
    return pl.pallas_call(
        kernel,
        out_shape=out,
        in_specs=ins,
        out_specs=tuple(VM() for _ in out) if many else VM(),
        scratch_shapes=list(scratch),
        compiler_params=pltpu.CompilerParams(**params),
        **kw,
    )


def vmem(*dims):
    return pltpu.VMEM(dims, F32)


def local(jacobians, residuals, camera_local, bucket_counts, camera_map):
    dma = pltpu.SemaphoreType.DMA
    part_b, part_g, part_e, inv = call(
        front_kernel,
        (shape(4, 2, 48, 128), shape(4, 2, 8, 128), shape(4, 2, 2, 128), shape(16, 128, dtype=jnp.int32)),
        [SM(), VM(), VM(), VM(), VM()],
        [
            vmem(64, 2, MSG, 128),
            vmem(64, 8, 128),
            vmem(64, 8, 128),
            vmem(HALF, 256),
        ]
        + [dma((64,))] * 4
        + [vmem(8, 2, MSG, 128)] * 8,
        cid=1,
        name="front",
    )(bucket_counts, jacobians, residuals, camera_local.reshape(256, 128), camera_map.reshape(512, 128))
    table, table_e, blocks = call(
        back_kernel,
        (shape(2 * SLOTS, 8, 128), shape(2 * SLOTS, 1, 128), shape(4, 2, 48, 128)),
        [SM(), VM(), VM(), VM()],
        [
            vmem(3, 2, 48, 128),
            vmem(3, 2, 8, 128),
            vmem(3, 2, 2, 128),
            vmem(2, 48, 128),
            vmem(4, 2, 48, 128),
            vmem(4, 2, 48, 128),
            vmem(2 * SLOTS + 8, 8, 128),
            vmem(2 * SLOTS + 8, 2, 128),
        ]
        + [dma((3,))] * 10
        + [dma((2, 8))] * 8,
        cid=2,
        name="back",
    )(inv, part_b, part_g, part_e)
    return pl.pallas_call(
        finish_kernel,
        out_shape=(shape(9, 65536), shape(81, 1024)),
        grid=(4,),
        in_specs=[
            pl.BlockSpec((2 * SLOTS // 4, 8, 128), lambda n: (n, 0, 0)),
            pl.BlockSpec((2 * SLOTS // 4, 1, 128), lambda n: (n, 0, 0)),
            pl.BlockSpec((1, 2, 48, 128), lambda n: (n, 0, 0, 0)),
        ],
        out_specs=(pl.BlockSpec((9, 16384), lambda n: (0, n)), pl.BlockSpec((81, 256), lambda n: (0, n))),
        name="finish",
    )(table, table_e, blocks)


def solution(mesh):
    return jax.shard_map(
        local,
        mesh=mesh,
        in_specs=(P(None, ("obs", "rep")), P(None, ("obs", "rep")), P(("obs", "rep")), P(("obs", "rep"), None), P()),
        out_specs=(P(), P(None, "obs")),
        check_vma=False,
    )
```

```python
import functools

import jax
import jax.numpy as jnp
from jax import lax
from jax.experimental import pallas as pl
from jax.experimental.pallas import tpu as pltpu
from jax.sharding import PartitionSpec as P

MESH = pl.DeviceIdType.MESH
F32 = jnp.float32
BF16 = jnp.bfloat16
CAP = 512
HALF = 512
ROWS = 56
MSG = 21
SLOTS = 256
VM = functools.partial(pl.BlockSpec, memory_space=pltpu.VMEM)
SM = functools.partial(pl.BlockSpec, memory_space=pltpu.SMEM)


def place():
    obs = lax.axis_index("obs")
    return obs // 8, (obs // 2) % 4, obs % 2, lax.axis_index("rep")


def bucket_of(z, y, core, x):
    return (2 * x + z % 2) * 8 + y * 2 + core


def terms(jac, res):
    j0, j1, r0, r1 = jac[0:9], jac[9:18], res[0:1], res[1:2]

    def turned(j, k):
        return j[0:8] if k == 0 else j[1:9] if k == 1 else jnp.concatenate([j[k:9], j[0 : k - 1]], axis=0)

    rows = [j0[0:8] * turned(j0, k) + j1[0:8] * turned(j1, k) for k in range(5)]
    last0 = jnp.concatenate([j0[8:9], j0[0:4], j0[0:2], r0], axis=0)
    last1 = jnp.concatenate([j1[8:9], j1[0:4], j1[0:2], r1], axis=0)
    rows.append(j0[8:9] * last0 + j1[8:9] * last1)
    rows.append(j0[0:8] * r0 + j1[0:8] * r1)
    return jnp.concatenate(rows, axis=0)


def weighted(jac, res, ids):
    full = terms(jac, res)
    high = full.astype(BF16).astype(F32)
    both = jnp.concatenate([high, full - high], axis=0)
    upper = ids >= HALF
    weights = jnp.concatenate([jnp.where(upper, 0.0, both), jnp.where(upper, both, 0.0)], axis=0)
    ids = jnp.where(upper, ids - HALF, ids)
    rows = lax.broadcasted_iota(jnp.int32, (HALF, ids.shape[1]), 0).astype(F32)
    hot = jnp.where(rows == ids, 1.0, 0.0).astype(BF16)
    return lax.dot_general(hot, weights.astype(BF16), (((1,), (1,)), ((), ())), preferred_element_type=F32)


def unfolded(acc_ref):
    turned = acc_ref[...].T
    low = turned[0:ROWS] + turned[ROWS : 2 * ROWS]
    high = turned[2 * ROWS : 3 * ROWS] + turned[3 * ROWS : 4 * ROWS]
    return low, high


def device_of(bucket, z):
    zd, y, core = bucket // 8, (bucket // 2) % 4, bucket % 2
    return ((z // 2) * 2 + zd % 2) * 8 + y * 2 + core, zd // 2


def slots_of(z, y, core, x):
    return core * 128 + x * 32 + y * 8 + z, core * 128 + y * 32 + x * 8 + z


def slot_of_camera(d, g):
    zd = d // 8
    return slots_of(2 * g + zd % 2, (d // 2) % 4, d % 2, zd // 2)


def at(z, y, core, x):
    return (z * 8 + y * 2 + core, x)


def remote(src, dst, send, recv, device):
    return pltpu.make_async_remote_copy(
        src_ref=src, dst_ref=dst, send_sem=send, recv_sem=recv, device_id=device, device_id_type=MESH
    )


def looped(start, stop, do):
    def body(i, c):
        do(i)
        return c

    lax.fori_loop(start, stop, body, 0)


def camera_ids_here(cam_map, hot):
    slots = slots_of(*place())
    bases = (slots[0] * 128, (SLOTS + slots[1]) * 128)
    lane = lax.broadcasted_iota(jnp.int32, (1, 128), 1)
    rows = lax.broadcasted_iota(jnp.int32, (16, 128), 0)
    chunk = 16

    def body(i, acc):
        left, right = [], []
        for k in range(chunk):
            r = i * chunk + k
            cam = r * 128 + lane
            first = cam_map[pl.ds(r, 1), :] - bases[0]
            second = cam_map[pl.ds(r, 1), :] - bases[1]
            inside = jnp.where((first >= 0) & (first < 128), first, -16)
            inside = jnp.where((second >= 0) & (second < 128), second + 128, inside)
            hit = rows == (inside >> 4)
            left.append(
                jnp.concatenate(
                    [jnp.where(hit, (cam >> 8).astype(F32), 0.0), jnp.where(hit, (cam & 255).astype(F32), 0.0)], axis=0
                )
            )
            right.append(jnp.where(rows == (inside & 15), 1.0, 0.0))
        a = jnp.concatenate(left, axis=1).astype(BF16)
        b = jnp.concatenate(right, axis=1).astype(BF16)
        return acc + lax.dot_general(a, b, (((1,), (1,)), ((), ())), preferred_element_type=F32)

    acc = lax.fori_loop(0, 512 // chunk, body, jnp.zeros((32, 16), F32))
    cam = (acc[0:16] * 256.0 + acc[16:32]).astype(jnp.int32) & (256 * SLOTS - 1)
    d, g, h, lane = cam >> 10, (cam >> 8) & 3, (cam >> 7) & 1, cam & 127
    zd, y, core = d >> 3, (d >> 1) & 3, d & 1
    slots = slots_of(2 * g + (zd & 1), y, core, zd >> 1)
    spot = jnp.where(h == 0, slots[0], SLOTS + slots[1])
    spot = jnp.where(d == hot, 2 * SLOTS + 2 * g + h, spot)
    return spot * 128 + lane


def sum_buckets(
    counts, jac, res, cam, cam_map, part_b, part_g, part_e, inv, msg, hots, gothot, acc, ssem, rsem, hssem, hrsem, gots
):
    chunk = 64 // len(gots)
    z, y, core, x = place()
    me = bucket_of(z, y, core, x)
    barrier = pltpu.get_barrier_semaphore()
    looped(
        1,
        64,
        lambda i: pl.semaphore_signal(
            barrier, inc=1, device_id=device_of((me + i) % 64, z), device_id_type=MESH
        ),
    )
    outside = [at(((z // 2) * 2 + i) % 8, y, core, x) for i in range(2, 8)]
    for peer in outside:
        pl.semaphore_signal(barrier, inc=1, device_id=peer, device_id_type=MESH)
    lane = lax.broadcasted_iota(jnp.int32, (1, 128), 1)

    def pack(d, carry):
        hot, ejac, eres, eids = carry
        live = counts[0, d]
        for h in range(2):
            col = pl.multiple_of(d * CAP + h * 128, 128)
            msg[d, h, 0:18, :] = jac[:, pl.ds(col, 128)]
            msg[d, h, 18:20, :] = res[:, pl.ds(col, 128)]
            ids = cam[pl.ds(d * 4 + h, 1), :]
            msg[d, h, 20:21, :] = jnp.where(lane + h * 128 < live, ids, -1).astype(F32)
        full = live == CAP
        col = pl.multiple_of(d * CAP + 256, 128)
        ids = jnp.concatenate([cam[pl.ds(d * 4 + 2, 1), :], cam[pl.ds(d * 4 + 3, 1), :]], axis=1)
        return (
            jnp.where(full, d, hot),
            jnp.where(full, jac[:, pl.ds(col, 256)], ejac),
            jnp.where(full, res[:, pl.ds(col, 256)], eres),
            jnp.where(full, ids, eids),
        )

    hot, ejac, eres, eids = lax.fori_loop(
        0,
        64,
        pack,
        (jnp.int32(0), jnp.zeros((18, 256), F32), jnp.zeros((2, 256), F32), jnp.zeros((1, 256), jnp.int32)),
    )
    pl.semaphore_wait(barrier, 63 + len(outside))

    def copy(i):
        to = (me + i) % 64
        return remote(msg.at[to], gots[(i - 1) // chunk].at[(i - 1) % chunk], ssem.at[i], rsem.at[i], device_of(to, z))

    def hot_copy(i):
        to = (me + i) % 64
        return remote(hots.at[to], gothot.at[i], hssem.at[i], hrsem.at[i], device_of(to, z))

    for i in range(1, 64):
        copy(i).start()
    gots[-1][chunk - 1] = msg[me]
    acc[:, 4 * ROWS :] = jnp.zeros((HALF, 256 - 4 * ROWS), F32)
    acc[:, : 4 * ROWS] = weighted(ejac, eres, eids.astype(F32))
    low, high = unfolded(acc)
    for q in range(4):
        hots[0:ROWS, q, :] = low[:, q * 128 : (q + 1) * 128]
        hots[0:ROWS, 4 + q, :] = high[:, q * 128 : (q + 1) * 128]
    hots[ROWS:64] = jnp.zeros((64 - ROWS, 8, 128), F32)
    for i in range(1, 64):
        hot_copy(i).start()
    gothot[0] = hots[me]
    inv[...] = jnp.zeros_like(inv)
    inv[:, 0:16] = camera_ids_here(cam_map, hot)
    inv[0:1, 16:17] = jnp.full((1, 1), hot, jnp.int32)

    acc[...] = jnp.zeros_like(acc)
    for c in range(64 // chunk):
        for i in range(c * chunk + 1, min(c * chunk + chunk + 1, 64)):
            copy(i).wait_recv()
        whole = jnp.concatenate([gots[c][s, h] for s in range(chunk) for h in range(2)], axis=1)
        acc[:, : 4 * ROWS] += weighted(whole[0:18], whole[18:20], whole[20:21])
    low, high = unfolded(acc)
    for i in range(1, 64):
        hot_copy(i).wait_recv()
    extra = lax.fori_loop(0, 64, lambda s, t: t + gothot[s], jnp.zeros((8, 128), F32))
    for g in range(4):
        part = low if g < 2 else high
        for h in range(2):
            q = (g % 2) * 2 + h
            tile = part[:, q * 128 : (q + 1) * 128]
            part_b[g, h] = tile[0:48]
            part_g[g, h] = tile[48:56]
            part_e[g, h, 0:1] = tile[47:48]
            part_e[g, h, 1:2] = extra[g * 2 + h : g * 2 + h + 1]

    def finish():
        for i in range(1, 64):
            copy(i).wait_send()
            hot_copy(i).wait_send()

    return finish


class Gather:
    def __init__(self, refs, sems):
        self.refs, self.sems = refs, sems
        z, y, core, x = place()
        self.slots = slots_of(z, y, core, x)
        ys = [at(z, (y + i) % 4, core, x) for i in range(1, 4)]
        xs = [at(z, y, core, (x + i) % 4) for i in range(1, 4)]
        self.zs = [at((z + i) % 8, y, core, x) for i in range(1, 8)]
        self.other = at(z, y, 1 - core, x)
        self.middle, self.last = (ys, xs), (xs, ys)
        self.mid, self.far = (y, x), (x, y)
        self.core = core

    def peers(self):
        return self.zs + self.middle[0] + self.middle[1] + [self.other]

    def copies(self, part, start, size, sem, device):
        out = []
        for n, ref in enumerate(self.refs):
            view = ref.at[pl.ds(part * SLOTS + start, size)]
            send, recv = self.sems[n]
            out.append(remote(view, view, send.at[part, sem], recv.at[part, sem], device))
        return out

    def start(self, *args):
        for c in self.copies(*args):
            c.start()

    def wait_recv(self, *args):
        for c in self.copies(*args):
            c.wait_recv()

    def run(self, between=()):
        between = list(between) + [lambda: None] * 4
        for part in range(2):
            for peer in self.zs:
                self.start(part, self.slots[part], 1, 0, peer)
        between[0]()
        blocks = [self.slots[part] // 8 * 8 for part in range(2)]
        for part in range(2):
            self.wait_recv(part, 0, 7, 0, self.zs[0])
            for i in range(3):
                self.start(part, blocks[part], 8, 1 + i, self.middle[part][i])
            for i in range(3):
                self.start(part, blocks[part], 8, 4 + i, self.last[part][i])
            self.start(part, blocks[part], 8, 7, self.other)
        between[1]()
        for i in range(3):
            for part in range(2):
                base = self.core * 128 + self.far[part] * 32 + (self.mid[part] + 3 - i) % 4 * 8
                self.wait_recv(part, base, 8, 1 + i, self.middle[part][i])
                for j in range(3):
                    self.start(part, base, 8, 4 + j, self.last[part][j])
                self.start(part, base, 8, 7, self.other)
        between[2]()
        for j in range(3):
            for part in range(2):
                base = self.core * 128 + (self.far[part] + 3 - j) % 4 * 32
                self.wait_recv(part, base, 32, 4 + j, self.last[part][j])
                self.start(part, base, 32, 7, self.other)
        between[3]()
        for part in range(2):
            self.wait_recv(part, 0, 128, 7, self.other)

    def finish(self):
        for part in range(2):
            for sem, size in [(0, 7)] + [(k, 8) for k in (1, 2, 3)] + [(k, 32) for k in (4, 5, 6)] + [(7, 128)]:
                for c in self.copies(part, 0, size, sem, self.other):
                    c.wait_send()


def main_kernel(
    counts, jac, res, cam, cam_map, table, table_e, blocks,
    part_b, part_g, part_e, found, inv, msg, hots, gothot, acc, ssem, rsem, hssem, hrsem, isem,
    got_b, got_g, got_e, mine_b, bx, bz, grad, grad_e,
    s2b, r2b, s2g, r2g, s2e, r2e, sx, rx, sz, rz, sg, rg, se, re, sg2, rg2, se2, re2,
    *gots,
):
    sums_sent = sum_buckets(
        counts, jac, res, cam, cam_map, part_b, part_g, part_e, found, msg, hots, gothot, acc, ssem, rsem, hssem, hrsem, gots
    )
    z, y, core, x = place()
    g, p = z // 2, z % 2
    first = Gather((grad, grad_e), ((sg, rg), (se, re)))
    second = Gather((table, table_e), ((sg2, rg2), (se2, re2)))
    ids = pltpu.make_async_copy(found, inv, isem)
    ids.start()

    small, large = [], []
    for i in range(1, 4):
        to = (g + i) % 4
        device = at(2 * to + p, y, core, x)
        small.append(remote(part_g.at[to], got_g.at[i - 1], s2g.at[i - 1], r2g.at[i - 1], device))
        small.append(remote(part_e.at[to], got_e.at[i - 1], s2e.at[i - 1], r2e.at[i - 1], device))
        large.append(remote(part_b.at[to], got_b.at[i - 1], s2b.at[i - 1], r2b.at[i - 1], device))
    for c in small:
        c.start()
    for c in small:
        c.wait_recv()
    total_g = part_g[g] + got_g[0] + got_g[1] + got_g[2]
    total_e = part_e[g] + got_e[0] + got_e[1] + got_e[2]
    for h in range(2):
        grad[h * SLOTS + first.slots[h]] = total_g[h]
        grad_e[h * SLOTS + first.slots[h]] = total_e[h]

    across, along = [], []
    for i in range(1, 4):
        across.append(remote(mine_b, bx.at[x], sx.at[i - 1], rx.at[i - 1], at(z, y, core, (x + i) % 4)))
        to = (g + i) % 4
        along.append(remote(bx.at[to], bz.at[g], sz.at[i - 1], rz.at[i - 1], at(2 * to + p, y, core, x)))

    def nothing():
        pass

    def start_blocks():
        for c in large:
            c.start()

    def spread_blocks():
        for c in large:
            c.wait_recv()
        mine_b[...] = part_b[g] + got_b[0] + got_b[1] + got_b[2]
        bx[x] = mine_b[...]
        for c in across:
            c.start()

    def send_blocks():
        for c in across:
            c.wait_recv()
        for c in along:
            c.start()
        bz[g] = bx[g]

    first.run([nothing, start_blocks])

    ids.wait()
    hot = inv[0, 16]
    for gg in range(4):
        hot_slots = slot_of_camera(hot, gg)
        for h in range(2):
            slot = h * SLOTS + hot_slots[h]
            extra = [grad_e[h * SLOTS + slot_of_camera(48 + k, gg)[h], 1:2] for k in range(8)]
            grad[2 * SLOTS + 2 * gg + h] = grad[slot] + jnp.concatenate(extra, axis=0)
            grad_e[2 * SLOTS + 2 * gg + h, 0:1] = (
                grad_e[slot, 0:1] + grad_e[h * SLOTS + slot_of_camera(47, gg)[h], 1:2]
            )
            grad_e[2 * SLOTS + 2 * gg + h, 1:2] = jnp.zeros((1, 128), F32)
    lane = lax.broadcasted_iota(jnp.int32, (1, 128), 1)
    for h in range(2):

        def pick(r, acc):
            top, low = acc
            for k in range(16):
                v = inv[h * 8 + r, k]
                q = r * 16 + k
                turn = (q - v) & 127
                at_q = lane == q
                top = jnp.where(at_q, pltpu.roll(grad[v >> 7], turn, 1), top)
                low = jnp.where(at_q, pltpu.roll(grad_e[v >> 7], turn, 1), low)
            return top, low

        top, low = lax.fori_loop(0, 8, pick, (jnp.zeros((8, 128), F32), jnp.zeros((2, 128), F32)))
        table[h * SLOTS + second.slots[h]] = top
        table_e[h * SLOTS + second.slots[h]] = low[0:1]

    def fix_blocks():
        for c in along:
            c.wait_recv()
        here = lax.axis_index("obs") == hot
        for gg in range(4):
            for h in range(2):
                extra = [grad_e[h * SLOTS + slot_of_camera(t, gg)[h], 1:2] for t in range(45)]
                extra = jnp.concatenate(extra + [jnp.zeros((3, 128), F32)], axis=0)
                blocks[gg, h] = bz[gg, h] + jnp.where(here, extra, 0.0)

    second.run([spread_blocks, send_blocks, nothing, fix_blocks])
    for c in small + large + across + along:
        c.wait_send()
    first.finish()
    second.finish()
    sums_sent()


def finish_kernel(table, table_e, blocks, out, blocks_out):
    for n in range(table.shape[0]):
        out[0:8, n * 128 : (n + 1) * 128] = table[n]
        out[8:9, n * 128 : (n + 1) * 128] = table_e[n]
    for h in range(2):
        whole = blocks[0, h]
        here = slice(h * 128, (h + 1) * 128)
        for k in range(9):
            for j in range(5):
                m = (k + j) % 9
                t = 40 + j if k == 8 else j * 8 + k
                blocks_out[k * 9 + m : k * 9 + m + 1, here] = whole[t : t + 1]
                if j:
                    blocks_out[m * 9 + k : m * 9 + k + 1, here] = whole[t : t + 1]


def shape(*dims, dtype=F32):
    return jax.ShapeDtypeStruct(dims, dtype)


def call(kernel, out, ins, scratch=(), cid=None, **kw):
    params = dict(vmem_limit_bytes=60 * 1024 * 1024)
    if cid is not None:
        params.update(collective_id=cid, has_side_effects=True)
    many = isinstance(out, tuple)
    return pl.pallas_call(
        kernel,
        out_shape=out,
        in_specs=ins,
        out_specs=tuple(VM() for _ in out) if many else VM(),
        scratch_shapes=list(scratch),
        compiler_params=pltpu.CompilerParams(**params),
        **kw,
    )


def vmem(*dims):
    return pltpu.VMEM(dims, F32)


def local(jacobians, residuals, camera_local, bucket_counts, camera_map):
    dma = pltpu.SemaphoreType.DMA
    table, table_e, blocks = call(
        main_kernel,
        (shape(2 * SLOTS, 8, 128), shape(2 * SLOTS, 1, 128), shape(4, 2, 48, 128)),
        [SM(), VM(), VM(), VM(), VM()],
        [
            vmem(4, 2, 48, 128),
            vmem(4, 2, 8, 128),
            vmem(4, 2, 2, 128),
            pltpu.VMEM((16, 128), jnp.int32),
            pltpu.SMEM((16, 128), jnp.int32),
            vmem(64, 2, MSG, 128),
            vmem(64, 8, 128),
            vmem(64, 8, 128),
            vmem(HALF, 256),
        ]
        + [dma((64,))] * 4
        + [
            dma,
            vmem(3, 2, 48, 128),
            vmem(3, 2, 8, 128),
            vmem(3, 2, 2, 128),
            vmem(2, 48, 128),
            vmem(4, 2, 48, 128),
            vmem(4, 2, 48, 128),
            vmem(2 * SLOTS + 8, 8, 128),
            vmem(2 * SLOTS + 8, 2, 128),
        ]
        + [dma((3,))] * 10
        + [dma((2, 8))] * 8
        + [vmem(8, 2, MSG, 128)] * 8,
        cid=1,
        name="main",
    )(bucket_counts, jacobians, residuals, camera_local.reshape(256, 128), camera_map.reshape(512, 128))
    return pl.pallas_call(
        finish_kernel,
        out_shape=(shape(9, 65536), shape(81, 1024)),
        grid=(4,),
        in_specs=[
            pl.BlockSpec((2 * SLOTS // 4, 8, 128), lambda n: (n, 0, 0)),
            pl.BlockSpec((2 * SLOTS // 4, 1, 128), lambda n: (n, 0, 0)),
            pl.BlockSpec((1, 2, 48, 128), lambda n: (n, 0, 0, 0)),
        ],
        out_specs=(pl.BlockSpec((9, 16384), lambda n: (0, n)), pl.BlockSpec((81, 256), lambda n: (0, n))),
        name="finish",
    )(table, table_e, blocks)


def solution(mesh):
    return jax.shard_map(
        local,
        mesh=mesh,
        in_specs=(P(None, ("obs", "rep")), P(None, ("obs", "rep")), P(("obs", "rep")), P(("obs", "rep"), None), P()),
        out_specs=(P(), P(None, "obs")),
        check_vma=False,
    )
```

```python
import functools

import jax
import jax.numpy as jnp
from jax import lax
from jax.experimental import pallas as pl
from jax.experimental.pallas import tpu as pltpu
from jax.sharding import PartitionSpec as P

MESH = pl.DeviceIdType.MESH
F32 = jnp.float32
BF16 = jnp.bfloat16
CAP = 512
HALF = 512
ROWS = 56
MSG = 21
SLOTS = 256
VM = functools.partial(pl.BlockSpec, memory_space=pltpu.VMEM)
SM = functools.partial(pl.BlockSpec, memory_space=pltpu.SMEM)


def place():
    obs = lax.axis_index("obs")
    return obs // 8, (obs // 2) % 4, obs % 2, lax.axis_index("rep")


def bucket_of(z, y, core, x):
    return (2 * x + z % 2) * 8 + y * 2 + core


def terms(jac, res):
    j0, j1, r0, r1 = jac[0:9], jac[9:18], res[0:1], res[1:2]

    def turned(j, k):
        return j[0:8] if k == 0 else j[1:9] if k == 1 else jnp.concatenate([j[k:9], j[0 : k - 1]], axis=0)

    rows = [j0[0:8] * turned(j0, k) + j1[0:8] * turned(j1, k) for k in range(5)]
    last0 = jnp.concatenate([j0[8:9], j0[0:4], j0[0:2], r0], axis=0)
    last1 = jnp.concatenate([j1[8:9], j1[0:4], j1[0:2], r1], axis=0)
    rows.append(j0[8:9] * last0 + j1[8:9] * last1)
    rows.append(j0[0:8] * r0 + j1[0:8] * r1)
    return jnp.concatenate(rows, axis=0)


def weighted(jac, res, ids):
    full = terms(jac, res)
    high = full.astype(BF16).astype(F32)
    both = jnp.concatenate([high, full - high], axis=0)
    upper = ids >= HALF
    weights = jnp.concatenate([jnp.where(upper, 0.0, both), jnp.where(upper, both, 0.0)], axis=0)
    ids = jnp.where(upper, ids - HALF, ids)
    rows = lax.broadcasted_iota(jnp.int32, (HALF, ids.shape[1]), 0).astype(F32)
    hot = jnp.where(rows == ids, 1.0, 0.0).astype(BF16)
    return lax.dot_general(hot, weights.astype(BF16), (((1,), (1,)), ((), ())), preferred_element_type=F32)


def unfolded(acc_ref):
    turned = acc_ref[...].T
    low = turned[0:ROWS] + turned[ROWS : 2 * ROWS]
    high = turned[2 * ROWS : 3 * ROWS] + turned[3 * ROWS : 4 * ROWS]
    return low, high


def device_of(bucket, z):
    zd, y, core = bucket // 8, (bucket // 2) % 4, bucket % 2
    return ((z // 2) * 2 + zd % 2) * 8 + y * 2 + core, zd // 2


def slots_of(z, y, core, x):
    return core * 128 + x * 32 + y * 8 + z, core * 128 + y * 32 + x * 8 + z


def slot_of_camera(d, g):
    zd = d // 8
    return slots_of(2 * g + zd % 2, (d // 2) % 4, d % 2, zd // 2)


def at(z, y, core, x):
    return (z * 8 + y * 2 + core, x)


def remote(src, dst, send, recv, device):
    return pltpu.make_async_remote_copy(
        src_ref=src, dst_ref=dst, send_sem=send, recv_sem=recv, device_id=device, device_id_type=MESH
    )


def looped(start, stop, do):
    def body(i, c):
        do(i)
        return c

    lax.fori_loop(start, stop, body, 0)


def camera_ids_here(cam_map, hot):
    slots = slots_of(*place())
    bases = (slots[0] * 128, (SLOTS + slots[1]) * 128)
    lane = lax.broadcasted_iota(jnp.int32, (1, 128), 1)
    rows = lax.broadcasted_iota(jnp.int32, (16, 128), 0)
    chunk = 16

    def body(i, acc):
        left, right = [], []
        for k in range(chunk):
            r = i * chunk + k
            cam = r * 128 + lane
            first = cam_map[pl.ds(r, 1), :] - bases[0]
            second = cam_map[pl.ds(r, 1), :] - bases[1]
            inside = jnp.where((first >= 0) & (first < 128), first, -16)
            inside = jnp.where((second >= 0) & (second < 128), second + 128, inside)
            hit = rows == (inside >> 4)
            left.append(
                jnp.concatenate(
                    [jnp.where(hit, (cam >> 8).astype(F32), 0.0), jnp.where(hit, (cam & 255).astype(F32), 0.0)], axis=0
                )
            )
            right.append(jnp.where(rows == (inside & 15), 1.0, 0.0))
        a = jnp.concatenate(left, axis=1).astype(BF16)
        b = jnp.concatenate(right, axis=1).astype(BF16)
        return acc + lax.dot_general(a, b, (((1,), (1,)), ((), ())), preferred_element_type=F32)

    acc = lax.fori_loop(0, 512 // chunk, body, jnp.zeros((32, 16), F32))
    cam = (acc[0:16] * 256.0 + acc[16:32]).astype(jnp.int32) & (256 * SLOTS - 1)
    d, g, h, lane = cam >> 10, (cam >> 8) & 3, (cam >> 7) & 1, cam & 127
    zd, y, core = d >> 3, (d >> 1) & 3, d & 1
    slots = slots_of(2 * g + (zd & 1), y, core, zd >> 1)
    spot = jnp.where(h == 0, slots[0], SLOTS + slots[1])
    spot = jnp.where(d == hot, 2 * SLOTS + 2 * g + h, spot)
    return spot * 128 + lane


def sum_buckets(
    counts, loads, jac, res, cam, cam_map, part_b, part_g, part_e, inv, msg, hots, gothot, acc, ssem, rsem, hssem, hrsem, gots
):
    chunk = 64 // len(gots)
    z, y, core, x = place()
    me = bucket_of(z, y, core, x)
    barrier = pltpu.get_barrier_semaphore()
    looped(
        1,
        64,
        lambda i: pl.semaphore_signal(
            barrier, inc=1, device_id=device_of((me + i) % 64, z), device_id_type=MESH
        ),
    )
    outside = [at(((z // 2) * 2 + i) % 8, y, core, x) for i in range(2, 8)]
    for peer in outside:
        pl.semaphore_signal(barrier, inc=1, device_id=peer, device_id_type=MESH)
    for c in loads:
        c.wait()
    lane = lax.broadcasted_iota(jnp.int32, (1, 128), 1)

    def pack(d, carry):
        hot, ejac, eres, eids = carry
        live = counts[0, d]
        for h in range(2):
            col = pl.multiple_of(d * CAP + h * 128, 128)
            msg[d, h, 0:18, :] = jac[:, pl.ds(col, 128)]
            msg[d, h, 18:20, :] = res[:, pl.ds(col, 128)]
            ids = cam[pl.ds(d * 4 + h, 1), :]
            msg[d, h, 20:21, :] = jnp.where(lane + h * 128 < live, ids, -1).astype(F32)
        full = live == CAP
        col = pl.multiple_of(d * CAP + 256, 128)
        ids = jnp.concatenate([cam[pl.ds(d * 4 + 2, 1), :], cam[pl.ds(d * 4 + 3, 1), :]], axis=1)
        return (
            jnp.where(full, d, hot),
            jnp.where(full, jac[:, pl.ds(col, 256)], ejac),
            jnp.where(full, res[:, pl.ds(col, 256)], eres),
            jnp.where(full, ids, eids),
        )

    hot, ejac, eres, eids = lax.fori_loop(
        0,
        64,
        pack,
        (jnp.int32(0), jnp.zeros((18, 256), F32), jnp.zeros((2, 256), F32), jnp.zeros((1, 256), jnp.int32)),
    )
    pl.semaphore_wait(barrier, 63 + len(outside))

    order = [(11 * k) % 64 for k in range(1, 64)]
    window = 24

    def copy(k):
        to = (me + order[k]) % 64
        return remote(msg.at[to], gots[k // chunk].at[k % chunk], ssem.at[k], rsem.at[k], device_of(to, z))

    def push(c):
        for k in range(c * chunk, min(c * chunk + chunk, 63)):
            if k >= window:
                copy(k - window).wait_send()
            copy(k).start()

    def hot_copy(i):
        to = (me + i) % 64
        return remote(hots.at[to], gothot.at[i], hssem.at[i], hrsem.at[i], device_of(to, z))

    for c in range(window // chunk):
        push(c)
    gots[-1][chunk - 1] = msg[me]
    acc[:, 4 * ROWS :] = jnp.zeros((HALF, 256 - 4 * ROWS), F32)
    acc[:, : 4 * ROWS] = weighted(ejac, eres, eids.astype(F32))
    low, high = unfolded(acc)
    for q in range(4):
        hots[0:ROWS, q, :] = low[:, q * 128 : (q + 1) * 128]
        hots[0:ROWS, 4 + q, :] = high[:, q * 128 : (q + 1) * 128]
    hots[ROWS:64] = jnp.zeros((64 - ROWS, 8, 128), F32)
    gothot[0] = hots[me]
    push(3)
    inv[...] = jnp.zeros_like(inv)
    inv[:, 0:16] = camera_ids_here(cam_map, hot)
    inv[0:1, 16:17] = jnp.full((1, 1), hot, jnp.int32)
    push(4)

    acc[...] = jnp.zeros_like(acc)
    for c in range(64 // chunk):
        for k in range(c * chunk, min(c * chunk + chunk, 63)):
            copy(k).wait_recv()
        whole = jnp.concatenate([gots[c][s, h] for s in range(chunk) for h in range(2)], axis=1)
        acc[:, : 4 * ROWS] += weighted(whole[0:18], whole[18:20], whole[20:21])
        if c < 3:
            push(5 + c)
        if c == 2:
            for i in range(1, 64):
                hot_copy(i).start()
    low, high = unfolded(acc)
    for i in range(1, 64):
        hot_copy(i).wait_recv()
    extra = lax.fori_loop(0, 64, lambda s, t: t + gothot[s], jnp.zeros((8, 128), F32))
    for g in range(4):
        part = low if g < 2 else high
        for h in range(2):
            q = (g % 2) * 2 + h
            tile = part[:, q * 128 : (q + 1) * 128]
            part_b[g, h] = tile[0:48]
            part_g[g, h] = tile[48:56]
            part_e[g, h, 0:1] = tile[47:48]
            part_e[g, h, 1:2] = extra[g * 2 + h : g * 2 + h + 1]

    def finish():
        for k in range(63 - window, 63):
            copy(k).wait_send()
        for i in range(1, 64):
            hot_copy(i).wait_send()

    return finish


class Gather:
    def __init__(self, refs, sems):
        self.refs, self.sems = refs, sems
        z, y, core, x = place()
        self.slots = slots_of(z, y, core, x)
        ys = [at(z, (y + i) % 4, core, x) for i in range(1, 4)]
        xs = [at(z, y, core, (x + i) % 4) for i in range(1, 4)]
        self.zs = [at((z + i) % 8, y, core, x) for i in (4, 3, 5, 2, 6, 1, 7)]
        self.other = at(z, y, 1 - core, x)
        self.middle, self.last = (ys, xs), (xs, ys)
        self.mid, self.far = (y, x), (x, y)
        self.core = core

    def peers(self):
        return self.zs + self.middle[0] + self.middle[1] + [self.other]

    def copies(self, part, start, size, sem, device):
        out = []
        for n, ref in enumerate(self.refs):
            view = ref.at[pl.ds(part * SLOTS + start, size)]
            send, recv = self.sems[n]
            out.append(remote(view, view, send.at[part, sem], recv.at[part, sem], device))
        return out

    def start(self, *args):
        for c in self.copies(*args):
            c.start()

    def wait_recv(self, *args):
        for c in self.copies(*args):
            c.wait_recv()

    def run(self, between=()):
        between = list(between) + [lambda: None] * 4
        for part in range(2):
            for peer in self.zs:
                self.start(part, self.slots[part], 1, 0, peer)
        between[0]()
        blocks = [self.slots[part] // 8 * 8 for part in range(2)]
        for part in range(2):
            self.wait_recv(part, 0, 7, 0, self.zs[0])
            for i in (1, 0, 2):
                self.start(part, blocks[part], 8, 1 + i, self.middle[part][i])
            for i in (1, 0, 2):
                self.start(part, blocks[part], 8, 4 + i, self.last[part][i])
            self.start(part, blocks[part], 8, 7, self.other)
        between[1]()
        for i in (0, 2, 1):
            for part in range(2):
                base = self.core * 128 + self.far[part] * 32 + (self.mid[part] + 3 - i) % 4 * 8
                self.wait_recv(part, base, 8, 1 + i, self.middle[part][i])
                for j in (1, 0, 2):
                    self.start(part, base, 8, 4 + j, self.last[part][j])
                self.start(part, base, 8, 7, self.other)
        between[2]()
        for j in (0, 2, 1):
            for part in range(2):
                base = self.core * 128 + (self.far[part] + 3 - j) % 4 * 32
                self.wait_recv(part, base, 32, 4 + j, self.last[part][j])
                self.start(part, base, 32, 7, self.other)
        between[3]()
        for part in range(2):
            self.wait_recv(part, 0, 128, 7, self.other)

    def finish(self):
        for part in range(2):
            for sem, size in [(0, 7)] + [(k, 8) for k in (1, 2, 3)] + [(k, 32) for k in (4, 5, 6)] + [(7, 128)]:
                for c in self.copies(part, 0, size, sem, self.other):
                    c.wait_send()


def main_kernel(
    counts, jac_far, res_far, cam_far, map_far, table, table_e, blocks,
    jac, res, cam, cam_map, lsem,
    part_b, part_g, part_e, found, inv, msg, hots, gothot, acc, ssem, rsem, hssem, hrsem, isem,
    got_b, got_g, got_e, mine_b, bx, bz, grad, grad_e,
    s2b, r2b, s2g, r2g, s2e, r2e, sx, rx, sz, rz, sg, rg, se, re, sg2, rg2, se2, re2,
    *gots,
):
    far = ((jac_far, jac), (res_far, res), (cam_far, cam), (map_far, cam_map))
    loads = [pltpu.make_async_copy(*pair, lsem.at[n]) for n, pair in enumerate(far)]
    for c in loads:
        c.start()
    sums_sent = sum_buckets(
        counts, loads, jac, res, cam, cam_map, part_b, part_g, part_e, found, msg, hots, gothot, acc, ssem, rsem, hssem, hrsem, gots
    )
    z, y, core, x = place()
    g, p = z // 2, z % 2
    first = Gather((grad, grad_e), ((sg, rg), (se, re)))
    second = Gather((table, table_e), ((sg2, rg2), (se2, re2)))
    ids = pltpu.make_async_copy(found, inv, isem)
    ids.start()

    small, large = [], []
    for i in range(1, 4):
        to = (g + i) % 4
        device = at(2 * to + p, y, core, x)
        small.append(remote(part_g.at[to], got_g.at[i - 1], s2g.at[i - 1], r2g.at[i - 1], device))
        small.append(remote(part_e.at[to], got_e.at[i - 1], s2e.at[i - 1], r2e.at[i - 1], device))
        large.append(remote(part_b.at[to], got_b.at[i - 1], s2b.at[i - 1], r2b.at[i - 1], device))
    for c in small:
        c.start()
    for c in small:
        c.wait_recv()
    total_g = part_g[g] + got_g[0] + got_g[1] + got_g[2]
    total_e = part_e[g] + got_e[0] + got_e[1] + got_e[2]
    for h in range(2):
        grad[h * SLOTS + first.slots[h]] = total_g[h]
        grad_e[h * SLOTS + first.slots[h]] = total_e[h]

    across, along = [], []
    for i in range(1, 4):
        across.append(remote(mine_b, bx.at[x], sx.at[i - 1], rx.at[i - 1], at(z, y, core, (x + i) % 4)))
        to = (g + i) % 4
        along.append(remote(bx.at[to], bz.at[g], sz.at[i - 1], rz.at[i - 1], at(2 * to + p, y, core, x)))

    def nothing():
        pass

    def start_blocks():
        for c in large:
            c.start()

    def spread_blocks():
        for c in large:
            c.wait_recv()
        mine_b[...] = part_b[g] + got_b[0] + got_b[1] + got_b[2]
        bx[x] = mine_b[...]
        for c in across:
            c.start()

    def send_blocks():
        for c in across:
            c.wait_recv()
        for c in along:
            c.start()
        bz[g] = bx[g]

    first.run([nothing, start_blocks])

    ids.wait()
    hot = inv[0, 16]
    for gg in range(4):
        hot_slots = slot_of_camera(hot, gg)
        for h in range(2):
            slot = h * SLOTS + hot_slots[h]
            extra = [grad_e[h * SLOTS + slot_of_camera(48 + k, gg)[h], 1:2] for k in range(8)]
            grad[2 * SLOTS + 2 * gg + h] = grad[slot] + jnp.concatenate(extra, axis=0)
            grad_e[2 * SLOTS + 2 * gg + h, 0:1] = (
                grad_e[slot, 0:1] + grad_e[h * SLOTS + slot_of_camera(47, gg)[h], 1:2]
            )
            grad_e[2 * SLOTS + 2 * gg + h, 1:2] = jnp.zeros((1, 128), F32)
    lane = lax.broadcasted_iota(jnp.int32, (1, 128), 1)
    for h in range(2):

        def pick(r, acc):
            top, low = acc
            for k in range(16):
                v = inv[h * 8 + r, k]
                q = r * 16 + k
                turn = (q - v) & 127
                at_q = lane == q
                top = jnp.where(at_q, pltpu.roll(grad[v >> 7], turn, 1), top)
                low = jnp.where(at_q, pltpu.roll(grad_e[v >> 7], turn, 1), low)
            return top, low

        top, low = lax.fori_loop(0, 8, pick, (jnp.zeros((8, 128), F32), jnp.zeros((2, 128), F32)))
        table[h * SLOTS + second.slots[h]] = top
        table_e[h * SLOTS + second.slots[h]] = low[0:1]

    def fix_blocks():
        for c in along:
            c.wait_recv()
        here = lax.axis_index("obs") == hot
        for gg in range(4):
            for h in range(2):
                extra = [grad_e[h * SLOTS + slot_of_camera(t, gg)[h], 1:2] for t in range(45)]
                extra = jnp.concatenate(extra + [jnp.zeros((3, 128), F32)], axis=0)
                blocks[gg, h] = bz[gg, h] + jnp.where(here, extra, 0.0)

    second.run([spread_blocks, send_blocks, nothing, fix_blocks])
    for c in small + large + across + along:
        c.wait_send()
    first.finish()
    second.finish()
    sums_sent()


def finish_kernel(table, table_e, blocks, out, blocks_out):
    for n in range(table.shape[0]):
        out[0:8, n * 128 : (n + 1) * 128] = table[n]
        out[8:9, n * 128 : (n + 1) * 128] = table_e[n]
    for h in range(2):
        whole = blocks[0, h]
        here = slice(h * 128, (h + 1) * 128)
        for k in range(9):
            for j in range(5):
                m = (k + j) % 9
                t = 40 + j if k == 8 else j * 8 + k
                blocks_out[k * 9 + m : k * 9 + m + 1, here] = whole[t : t + 1]
                if j:
                    blocks_out[m * 9 + k : m * 9 + k + 1, here] = whole[t : t + 1]


def shape(*dims, dtype=F32):
    return jax.ShapeDtypeStruct(dims, dtype)


def call(kernel, out, ins, scratch=(), cid=None, **kw):
    params = dict(vmem_limit_bytes=60 * 1024 * 1024)
    if cid is not None:
        params.update(collective_id=cid, has_side_effects=True)
    many = isinstance(out, tuple)
    return pl.pallas_call(
        kernel,
        out_shape=out,
        in_specs=ins,
        out_specs=tuple(VM() for _ in out) if many else VM(),
        scratch_shapes=list(scratch),
        compiler_params=pltpu.CompilerParams(**params),
        **kw,
    )


def vmem(*dims):
    return pltpu.VMEM(dims, F32)


def local(jacobians, residuals, camera_local, bucket_counts, camera_map):
    dma = pltpu.SemaphoreType.DMA
    table, table_e, blocks = call(
        main_kernel,
        (shape(2 * SLOTS, 8, 128), shape(2 * SLOTS, 1, 128), shape(4, 2, 48, 128)),
        [SM()] + [pl.BlockSpec(memory_space=pl.ANY)] * 4,
        [
            vmem(18, 32768),
            vmem(2, 32768),
            pltpu.VMEM((256, 128), jnp.int32),
            pltpu.VMEM((512, 128), jnp.int32),
            dma((4,)),
            vmem(4, 2, 48, 128),
            vmem(4, 2, 8, 128),
            vmem(4, 2, 2, 128),
            pltpu.VMEM((16, 128), jnp.int32),
            pltpu.SMEM((16, 128), jnp.int32),
            vmem(64, 2, MSG, 128),
            vmem(64, 8, 128),
            vmem(64, 8, 128),
            vmem(HALF, 256),
        ]
        + [dma((64,))] * 4
        + [
            dma,
            vmem(3, 2, 48, 128),
            vmem(3, 2, 8, 128),
            vmem(3, 2, 2, 128),
            vmem(2, 48, 128),
            vmem(4, 2, 48, 128),
            vmem(4, 2, 48, 128),
            vmem(2 * SLOTS + 8, 8, 128),
            vmem(2 * SLOTS + 8, 2, 128),
        ]
        + [dma((3,))] * 10
        + [dma((2, 8))] * 8
        + [vmem(8, 2, MSG, 128)] * 8,
        cid=1,
        name="main",
    )(bucket_counts, jacobians, residuals, camera_local.reshape(256, 128), camera_map.reshape(512, 128))
    return pl.pallas_call(
        finish_kernel,
        out_shape=(shape(9, 65536), shape(81, 1024)),
        grid=(4,),
        in_specs=[
            pl.BlockSpec((2 * SLOTS // 4, 8, 128), lambda n: (n, 0, 0)),
            pl.BlockSpec((2 * SLOTS // 4, 1, 128), lambda n: (n, 0, 0)),
            pl.BlockSpec((1, 2, 48, 128), lambda n: (n, 0, 0, 0)),
        ],
        out_specs=(pl.BlockSpec((9, 16384), lambda n: (0, n)), pl.BlockSpec((81, 256), lambda n: (0, n))),
        name="finish",
    )(table, table_e, blocks)


def solution(mesh):
    return jax.shard_map(
        local,
        mesh=mesh,
        in_specs=(P(None, ("obs", "rep")), P(None, ("obs", "rep")), P(("obs", "rep")), P(("obs", "rep"), None), P()),
        out_specs=(P(), P(None, "obs")),
        check_vma=False,
    )
```

```python
import functools

import jax
import jax.numpy as jnp
from jax import lax
from jax.experimental import pallas as pl
from jax.experimental.pallas import tpu as pltpu
from jax.sharding import PartitionSpec as P

MESH = pl.DeviceIdType.MESH
F32 = jnp.float32
BF16 = jnp.bfloat16
CAP = 512
HALF = 512
ROWS = 56
MSG = 21
SLOTS = 256
VM = functools.partial(pl.BlockSpec, memory_space=pltpu.VMEM)
SM = functools.partial(pl.BlockSpec, memory_space=pltpu.SMEM)


def place():
    obs = lax.axis_index("obs")
    return obs // 8, (obs // 2) % 4, obs % 2, lax.axis_index("rep")


def bucket_of(z, y, core, x):
    return (2 * x + z % 2) * 8 + y * 2 + core


def terms(jac, res):
    j0, j1, r0, r1 = jac[0:9], jac[9:18], res[0:1], res[1:2]

    def turned(j, k):
        return j[0:8] if k == 0 else j[1:9] if k == 1 else jnp.concatenate([j[k:9], j[0 : k - 1]], axis=0)

    rows = [j0[0:8] * turned(j0, k) + j1[0:8] * turned(j1, k) for k in range(5)]
    last0 = jnp.concatenate([j0[8:9], j0[0:4], j0[0:2], r0], axis=0)
    last1 = jnp.concatenate([j1[8:9], j1[0:4], j1[0:2], r1], axis=0)
    rows.append(j0[8:9] * last0 + j1[8:9] * last1)
    rows.append(j0[0:8] * r0 + j1[0:8] * r1)
    return jnp.concatenate(rows, axis=0)


def weighted(jac, res, ids):
    full = terms(jac, res)
    high = full.astype(BF16).astype(F32)
    both = jnp.concatenate([high, full - high], axis=0)
    upper = ids >= HALF
    weights = jnp.concatenate([jnp.where(upper, 0.0, both), jnp.where(upper, both, 0.0)], axis=0)
    ids = jnp.where(upper, ids - HALF, ids)
    rows = lax.broadcasted_iota(jnp.int32, (HALF, ids.shape[1]), 0).astype(F32)
    hot = jnp.where(rows == ids, 1.0, 0.0).astype(BF16)
    return lax.dot_general(hot, weights.astype(BF16), (((1,), (1,)), ((), ())), preferred_element_type=F32)


def unfolded(acc_ref):
    turned = acc_ref[...].T
    low = turned[0:ROWS] + turned[ROWS : 2 * ROWS]
    high = turned[2 * ROWS : 3 * ROWS] + turned[3 * ROWS : 4 * ROWS]
    return low, high


def device_of(bucket, z):
    zd, y, core = bucket // 8, (bucket // 2) % 4, bucket % 2
    return ((z // 2) * 2 + zd % 2) * 8 + y * 2 + core, zd // 2


def slots_of(z, y, core, x):
    return core * 128 + x * 32 + y * 8 + z, core * 128 + y * 32 + x * 8 + z


def slot_of_camera(d, g):
    zd = d // 8
    return slots_of(2 * g + zd % 2, (d // 2) % 4, d % 2, zd // 2)


def at(z, y, core, x):
    return (z * 8 + y * 2 + core, x)


def remote(src, dst, send, recv, device):
    return pltpu.make_async_remote_copy(
        src_ref=src, dst_ref=dst, send_sem=send, recv_sem=recv, device_id=device, device_id_type=MESH
    )


def looped(start, stop, do):
    def body(i, c):
        do(i)
        return c

    lax.fori_loop(start, stop, body, 0)


def camera_ids_here(cam_map, hot):
    slots = slots_of(*place())
    bases = (slots[0] * 128, (SLOTS + slots[1]) * 128)
    lane = lax.broadcasted_iota(jnp.int32, (1, 128), 1)
    rows = lax.broadcasted_iota(jnp.int32, (16, 128), 0)
    chunk = 16

    def body(i, acc):
        left, right = [], []
        for k in range(chunk):
            r = i * chunk + k
            cam = r * 128 + lane
            first = cam_map[pl.ds(r, 1), :] - bases[0]
            second = cam_map[pl.ds(r, 1), :] - bases[1]
            inside = jnp.where((first >= 0) & (first < 128), first, -16)
            inside = jnp.where((second >= 0) & (second < 128), second + 128, inside)
            hit = rows == (inside >> 4)
            left.append(
                jnp.concatenate(
                    [jnp.where(hit, (cam >> 8).astype(F32), 0.0), jnp.where(hit, (cam & 255).astype(F32), 0.0)], axis=0
                )
            )
            right.append(jnp.where(rows == (inside & 15), 1.0, 0.0))
        a = jnp.concatenate(left, axis=1).astype(BF16)
        b = jnp.concatenate(right, axis=1).astype(BF16)
        return acc + lax.dot_general(a, b, (((1,), (1,)), ((), ())), preferred_element_type=F32)

    acc = lax.fori_loop(0, 512 // chunk, body, jnp.zeros((32, 16), F32))
    cam = (acc[0:16] * 256.0 + acc[16:32]).astype(jnp.int32) & (256 * SLOTS - 1)
    d, g, h, lane = cam >> 10, (cam >> 8) & 3, (cam >> 7) & 1, cam & 127
    zd, y, core = d >> 3, (d >> 1) & 3, d & 1
    slots = slots_of(2 * g + (zd & 1), y, core, zd >> 1)
    spot = jnp.where(h == 0, slots[0], SLOTS + slots[1])
    spot = jnp.where(d == hot, 2 * SLOTS + 2 * g + h, spot)
    return spot * 128 + lane


def sum_buckets(
    counts, loads, jac, res, cam, cam_map, part_b, part_g, part_e, inv, msg, hots, gothot, acc, ssem, rsem, hssem, hrsem, gots
):
    chunk = 64 // len(gots)
    z, y, core, x = place()
    me = bucket_of(z, y, core, x)
    barrier = pltpu.get_barrier_semaphore()
    looped(
        1,
        64,
        lambda i: pl.semaphore_signal(
            barrier, inc=1, device_id=device_of((me + i) % 64, z), device_id_type=MESH
        ),
    )
    outside = [at(((z // 2) * 2 + i) % 8, y, core, x) for i in range(2, 8)]
    for peer in outside:
        pl.semaphore_signal(barrier, inc=1, device_id=peer, device_id_type=MESH)
    for c in loads:
        c.wait()
    lane = lax.broadcasted_iota(jnp.int32, (1, 128), 1)

    def pack(d, carry):
        hot, ejac, eres, eids = carry
        live = counts[0, d]
        for h in range(2):
            col = pl.multiple_of(d * CAP + h * 128, 128)
            msg[d, h, 0:18, :] = jac[:, pl.ds(col, 128)]
            msg[d, h, 18:20, :] = res[:, pl.ds(col, 128)]
            ids = cam[pl.ds(d * 4 + h, 1), :]
            msg[d, h, 20:21, :] = jnp.where(lane + h * 128 < live, ids, -1).astype(F32)
        full = live == CAP
        col = pl.multiple_of(d * CAP + 256, 128)
        ids = jnp.concatenate([cam[pl.ds(d * 4 + 2, 1), :], cam[pl.ds(d * 4 + 3, 1), :]], axis=1)
        return (
            jnp.where(full, d, hot),
            jnp.where(full, jac[:, pl.ds(col, 256)], ejac),
            jnp.where(full, res[:, pl.ds(col, 256)], eres),
            jnp.where(full, ids, eids),
        )

    hot, ejac, eres, eids = lax.fori_loop(
        0,
        64,
        pack,
        (jnp.int32(0), jnp.zeros((18, 256), F32), jnp.zeros((2, 256), F32), jnp.zeros((1, 256), jnp.int32)),
    )
    pl.semaphore_wait(barrier, 63 + len(outside))

    order = [(11 * k) % 64 for k in range(1, 64)]
    window = 24

    def copy(k):
        to = (me + order[k]) % 64
        return remote(msg.at[to], gots[k // chunk].at[k % chunk], ssem.at[k], rsem.at[k], device_of(to, z))

    def push(c):
        for k in range(c * chunk, min(c * chunk + chunk, 63)):
            if k >= window:
                copy(k - window).wait_send()
            copy(k).start()

    def hot_copy(i):
        to = (me + i) % 64
        return remote(hots.at[to], gothot.at[i], hssem.at[i], hrsem.at[i], device_of(to, z))

    for c in range(window // chunk):
        push(c)
    gots[-1][chunk - 1] = msg[me]
    acc[:, 4 * ROWS :] = jnp.zeros((HALF, 256 - 4 * ROWS), F32)
    acc[:, : 4 * ROWS] = weighted(ejac, eres, eids.astype(F32))
    low, high = unfolded(acc)
    for q in range(4):
        hots[0:ROWS, q, :] = low[:, q * 128 : (q + 1) * 128]
        hots[0:ROWS, 4 + q, :] = high[:, q * 128 : (q + 1) * 128]
    hots[ROWS:64] = jnp.zeros((64 - ROWS, 8, 128), F32)
    gothot[0] = hots[me]
    push(3)
    inv[...] = jnp.zeros_like(inv)
    inv[:, 0:16] = camera_ids_here(cam_map, hot)
    inv[0:1, 16:17] = jnp.full((1, 1), hot, jnp.int32)
    push(4)

    acc[...] = jnp.zeros_like(acc)
    for c in range(64 // chunk):
        for k in range(c * chunk, min(c * chunk + chunk, 63)):
            copy(k).wait_recv()
        whole = jnp.concatenate([gots[c][s, h] for s in range(chunk) for h in range(2)], axis=1)
        acc[:, : 4 * ROWS] += weighted(whole[0:18], whole[18:20], whole[20:21])
        if c < 3:
            push(5 + c)
        if c == 2:
            for i in range(1, 64):
                hot_copy(i).start()
    low, high = unfolded(acc)
    for i in range(1, 64):
        hot_copy(i).wait_recv()
    extra = lax.fori_loop(0, 64, lambda s, t: t + gothot[s], jnp.zeros((8, 128), F32))
    for g in range(4):
        part = low if g < 2 else high
        for h in range(2):
            q = (g % 2) * 2 + h
            tile = part[:, q * 128 : (q + 1) * 128]
            part_b[g, h] = tile[0:48]
            part_g[g, h] = tile[48:56]
            part_e[g, h, 0:1] = tile[47:48]
            part_e[g, h, 1:2] = extra[g * 2 + h : g * 2 + h + 1]

    def finish():
        for k in range(63 - window, 63):
            copy(k).wait_send()
        for i in range(1, 64):
            hot_copy(i).wait_send()

    return finish


class Gather:
    def __init__(self, refs, sems):
        self.refs, self.sems = refs, sems
        z, y, core, x = place()
        self.slots = slots_of(z, y, core, x)
        ys = [at(z, (y + i) % 4, core, x) for i in range(1, 4)]
        xs = [at(z, y, core, (x + i) % 4) for i in range(1, 4)]
        self.steps = (4, 3, 5, 2, 6, 1, 7)
        self.zs = [at((z + i) % 8, y, core, x) for i in self.steps]
        self.other = at(z, y, 1 - core, x)
        self.middle, self.last = (ys, xs), (xs, ys)
        self.mid, self.far = (y, x), (x, y)
        self.core = core

    def peers(self):
        return self.zs + self.middle[0] + self.middle[1] + [self.other]

    def copies(self, part, start, size, sem, device):
        out = []
        for n, ref in enumerate(self.refs):
            view = ref.at[pl.ds(part * SLOTS + start, size)]
            send, recv = self.sems[n]
            out.append(remote(view, view, send.at[part, sem], recv.at[part, sem], device))
        return out

    def start(self, *args):
        for c in self.copies(*args):
            c.start()

    def wait_recv(self, *args):
        for c in self.copies(*args):
            c.wait_recv()

    def forward(self, part, slot):
        for i in (1, 0, 2):
            self.start(part, slot, 1, 1 + i, self.middle[part][i])
        for i in (1, 0, 2):
            self.start(part, slot, 1, 4 + i, self.last[part][i])
        self.start(part, slot, 1, 7, self.other)

    def run(self, between=()):
        between = list(between) + [lambda: None] * 4
        for part in range(2):
            for n, peer in enumerate(self.zs):
                self.start(part, self.slots[part], 1, 8 + n, peer)
        for part in range(2):
            self.forward(part, self.slots[part])
        between[0]()
        for n in (6, 5, 4, 3, 2, 1, 0):
            for part in range(2):
                slot = self.slots[part] // 8 * 8 + (self.slots[part] + 8 - self.steps[n]) % 8
                self.wait_recv(part, slot, 1, 8 + n, self.zs[n])
                self.forward(part, slot)
        between[1]()
        for i in (0, 2, 1):
            for part in range(2):
                base = self.core * 128 + self.far[part] * 32 + (self.mid[part] + 3 - i) % 4 * 8
                self.wait_recv(part, base, 8, 1 + i, self.middle[part][i])
                for j in (1, 0, 2):
                    self.start(part, base, 8, 4 + j, self.last[part][j])
                self.start(part, base, 8, 7, self.other)
        between[2]()
        for j in (0, 2, 1):
            for part in range(2):
                base = self.core * 128 + (self.far[part] + 3 - j) % 4 * 32
                self.wait_recv(part, base, 32, 4 + j, self.last[part][j])
                self.start(part, base, 32, 7, self.other)
        between[3]()
        for part in range(2):
            self.wait_recv(part, 0, 128, 7, self.other)

    def finish(self):
        for part in range(2):
            for sem, size in [(8 + k, 1) for k in range(7)] + [(k, 8) for k in (1, 2, 3)] + [(k, 32) for k in (4, 5, 6)] + [(7, 128)]:
                for c in self.copies(part, 0, size, sem, self.other):
                    c.wait_send()


def main_kernel(
    counts, jac_far, res_far, cam_far, map_far, table, table_e, blocks,
    jac, res, cam, cam_map, lsem,
    part_b, part_g, part_e, found, inv, msg, hots, gothot, acc, ssem, rsem, hssem, hrsem, isem,
    got_b, got_g, got_e, mine_b, bx, bz, grad, grad_e,
    s2b, r2b, s2g, r2g, s2e, r2e, sx, rx, sz, rz, sg, rg, se, re, sg2, rg2, se2, re2,
    *gots,
):
    far = ((jac_far, jac), (res_far, res), (cam_far, cam), (map_far, cam_map))
    loads = [pltpu.make_async_copy(*pair, lsem.at[n]) for n, pair in enumerate(far)]
    for c in loads:
        c.start()
    sums_sent = sum_buckets(
        counts, loads, jac, res, cam, cam_map, part_b, part_g, part_e, found, msg, hots, gothot, acc, ssem, rsem, hssem, hrsem, gots
    )
    z, y, core, x = place()
    g, p = z // 2, z % 2
    first = Gather((grad, grad_e), ((sg, rg), (se, re)))
    second = Gather((table, table_e), ((sg2, rg2), (se2, re2)))
    ids = pltpu.make_async_copy(found, inv, isem)
    ids.start()

    small, large = [], []
    for i in range(1, 4):
        to = (g + i) % 4
        device = at(2 * to + p, y, core, x)
        small.append(remote(part_g.at[to], got_g.at[i - 1], s2g.at[i - 1], r2g.at[i - 1], device))
        small.append(remote(part_e.at[to], got_e.at[i - 1], s2e.at[i - 1], r2e.at[i - 1], device))
        large.append(remote(part_b.at[to], got_b.at[i - 1], s2b.at[i - 1], r2b.at[i - 1], device))
    for c in small:
        c.start()
    for c in small:
        c.wait_recv()
    total_g = part_g[g] + got_g[0] + got_g[1] + got_g[2]
    total_e = part_e[g] + got_e[0] + got_e[1] + got_e[2]
    for h in range(2):
        grad[h * SLOTS + first.slots[h]] = total_g[h]
        grad_e[h * SLOTS + first.slots[h]] = total_e[h]

    across, along = [], []
    for i in range(1, 4):
        across.append(remote(mine_b, bx.at[x], sx.at[i - 1], rx.at[i - 1], at(z, y, core, (x + i) % 4)))
        to = (g + i) % 4
        along.append(remote(bx.at[to], bz.at[g], sz.at[i - 1], rz.at[i - 1], at(2 * to + p, y, core, x)))

    def nothing():
        pass

    def start_blocks():
        for c in large:
            c.start()

    def spread_blocks():
        for c in large:
            c.wait_recv()
        mine_b[...] = part_b[g] + got_b[0] + got_b[1] + got_b[2]
        bx[x] = mine_b[...]
        for c in across:
            c.start()

    def send_blocks():
        for c in across:
            c.wait_recv()
        for c in along:
            c.start()
        bz[g] = bx[g]

    first.run([nothing, start_blocks])

    ids.wait()
    hot = inv[0, 16]
    for gg in range(4):
        hot_slots = slot_of_camera(hot, gg)
        for h in range(2):
            slot = h * SLOTS + hot_slots[h]
            extra = [grad_e[h * SLOTS + slot_of_camera(48 + k, gg)[h], 1:2] for k in range(8)]
            grad[2 * SLOTS + 2 * gg + h] = grad[slot] + jnp.concatenate(extra, axis=0)
            grad_e[2 * SLOTS + 2 * gg + h, 0:1] = (
                grad_e[slot, 0:1] + grad_e[h * SLOTS + slot_of_camera(47, gg)[h], 1:2]
            )
            grad_e[2 * SLOTS + 2 * gg + h, 1:2] = jnp.zeros((1, 128), F32)
    lane = lax.broadcasted_iota(jnp.int32, (1, 128), 1)
    for h in range(2):

        def pick(r, acc):
            top, low = acc
            for k in range(64):
                v = inv[h * 8 + r * 4 + k // 16, k % 16]
                q = r * 64 + k
                turn = (q - v) & 127
                at_q = lane == q
                top = jnp.where(at_q, pltpu.roll(grad[v >> 7], turn, 1), top)
                low = jnp.where(at_q, pltpu.roll(grad_e[v >> 7], turn, 1), low)
            return top, low

        top, low = lax.fori_loop(0, 2, pick, (jnp.zeros((8, 128), F32), jnp.zeros((2, 128), F32)))
        table[h * SLOTS + second.slots[h]] = top
        table_e[h * SLOTS + second.slots[h]] = low[0:1]

    def fix_blocks():
        for c in along:
            c.wait_recv()
        here = lax.axis_index("obs") == hot
        for gg in range(4):
            for h in range(2):
                extra = [grad_e[h * SLOTS + slot_of_camera(t, gg)[h], 1:2] for t in range(45)]
                extra = jnp.concatenate(extra + [jnp.zeros((3, 128), F32)], axis=0)
                blocks[gg, h] = bz[gg, h] + jnp.where(here, extra, 0.0)

    second.run([spread_blocks, send_blocks, nothing, fix_blocks])
    for c in small + large + across + along:
        c.wait_send()
    first.finish()
    second.finish()
    sums_sent()


def finish_kernel(table, table_e, blocks, out, blocks_out):
    for n in range(table.shape[0]):
        out[0:8, n * 128 : (n + 1) * 128] = table[n]
        out[8:9, n * 128 : (n + 1) * 128] = table_e[n]
    for h in range(2):
        whole = blocks[0, h]
        here = slice(h * 128, (h + 1) * 128)
        for k in range(9):
            for j in range(5):
                m = (k + j) % 9
                t = 40 + j if k == 8 else j * 8 + k
                blocks_out[k * 9 + m : k * 9 + m + 1, here] = whole[t : t + 1]
                if j:
                    blocks_out[m * 9 + k : m * 9 + k + 1, here] = whole[t : t + 1]


def shape(*dims, dtype=F32):
    return jax.ShapeDtypeStruct(dims, dtype)


def call(kernel, out, ins, scratch=(), cid=None, **kw):
    params = dict(vmem_limit_bytes=60 * 1024 * 1024)
    if cid is not None:
        params.update(collective_id=cid, has_side_effects=True)
    many = isinstance(out, tuple)
    return pl.pallas_call(
        kernel,
        out_shape=out,
        in_specs=ins,
        out_specs=tuple(VM() for _ in out) if many else VM(),
        scratch_shapes=list(scratch),
        compiler_params=pltpu.CompilerParams(**params),
        **kw,
    )


def vmem(*dims):
    return pltpu.VMEM(dims, F32)


def local(jacobians, residuals, camera_local, bucket_counts, camera_map):
    dma = pltpu.SemaphoreType.DMA
    table, table_e, blocks = call(
        main_kernel,
        (shape(2 * SLOTS, 8, 128), shape(2 * SLOTS, 1, 128), shape(4, 2, 48, 128)),
        [SM()] + [pl.BlockSpec(memory_space=pl.ANY)] * 4,
        [
            vmem(18, 32768),
            vmem(2, 32768),
            pltpu.VMEM((256, 128), jnp.int32),
            pltpu.VMEM((512, 128), jnp.int32),
            dma((4,)),
            vmem(4, 2, 48, 128),
            vmem(4, 2, 8, 128),
            vmem(4, 2, 2, 128),
            pltpu.VMEM((16, 128), jnp.int32),
            pltpu.SMEM((16, 128), jnp.int32),
            vmem(64, 2, MSG, 128),
            vmem(64, 8, 128),
            vmem(64, 8, 128),
            vmem(HALF, 256),
        ]
        + [dma((64,))] * 4
        + [
            dma,
            vmem(3, 2, 48, 128),
            vmem(3, 2, 8, 128),
            vmem(3, 2, 2, 128),
            vmem(2, 48, 128),
            vmem(4, 2, 48, 128),
            vmem(4, 2, 48, 128),
            vmem(2 * SLOTS + 8, 8, 128),
            vmem(2 * SLOTS + 8, 2, 128),
        ]
        + [dma((3,))] * 10
        + [dma((2, 16))] * 8
        + [vmem(8, 2, MSG, 128)] * 8,
        cid=1,
        name="main",
    )(bucket_counts, jacobians, residuals, camera_local.reshape(256, 128), camera_map.reshape(512, 128))
    return pl.pallas_call(
        finish_kernel,
        out_shape=(shape(9, 65536), shape(81, 1024)),
        grid=(4,),
        in_specs=[
            pl.BlockSpec((2 * SLOTS // 4, 8, 128), lambda n: (n, 0, 0)),
            pl.BlockSpec((2 * SLOTS // 4, 1, 128), lambda n: (n, 0, 0)),
            pl.BlockSpec((1, 2, 48, 128), lambda n: (n, 0, 0, 0)),
        ],
        out_specs=(pl.BlockSpec((9, 16384), lambda n: (0, n)), pl.BlockSpec((81, 256), lambda n: (0, n))),
        name="finish",
    )(table, table_e, blocks)


def solution(mesh):
    return jax.shard_map(
        local,
        mesh=mesh,
        in_specs=(P(None, ("obs", "rep")), P(None, ("obs", "rep")), P(("obs", "rep")), P(("obs", "rep"), None), P()),
        out_specs=(P(), P(None, "obs")),
        check_vma=False,
    )
```

```python
import functools

import jax
import jax.numpy as jnp
from jax import lax
from jax.experimental import pallas as pl
from jax.experimental.pallas import tpu as pltpu
from jax.sharding import PartitionSpec as P

MESH = pl.DeviceIdType.MESH
F32 = jnp.float32
BF16 = jnp.bfloat16
CAP = 512
HALF = 512
ROWS = 56
MSG = 21
SLOTS = 256
VM = functools.partial(pl.BlockSpec, memory_space=pltpu.VMEM)
SM = functools.partial(pl.BlockSpec, memory_space=pltpu.SMEM)


def place():
    obs = lax.axis_index("obs")
    return obs // 8, (obs // 2) % 4, obs % 2, lax.axis_index("rep")


def bucket_of(z, y, core, x):
    return (2 * x + z % 2) * 8 + y * 2 + core


def terms(jac, res):
    j0, j1, r0, r1 = jac[0:9], jac[9:18], res[0:1], res[1:2]

    def turned(j, k):
        return j[0:8] if k == 0 else j[1:9] if k == 1 else jnp.concatenate([j[k:9], j[0 : k - 1]], axis=0)

    rows = [j0[0:8] * turned(j0, k) + j1[0:8] * turned(j1, k) for k in range(5)]
    last0 = jnp.concatenate([j0[8:9], j0[0:4], j0[0:2], r0], axis=0)
    last1 = jnp.concatenate([j1[8:9], j1[0:4], j1[0:2], r1], axis=0)
    rows.append(j0[8:9] * last0 + j1[8:9] * last1)
    rows.append(j0[0:8] * r0 + j1[0:8] * r1)
    return jnp.concatenate(rows, axis=0)


def weighted(jac, res, ids):
    full = terms(jac, res)
    high = full.astype(BF16).astype(F32)
    both = jnp.concatenate([high, full - high], axis=0)
    upper = ids >= HALF
    weights = jnp.concatenate([jnp.where(upper, 0.0, both), jnp.where(upper, both, 0.0)], axis=0)
    ids = jnp.where(upper, ids - HALF, ids)
    rows = lax.broadcasted_iota(jnp.int32, (HALF, ids.shape[1]), 0).astype(F32)
    hot = jnp.where(rows == ids, 1.0, 0.0).astype(BF16)
    return lax.dot_general(hot, weights.astype(BF16), (((1,), (1,)), ((), ())), preferred_element_type=F32)


def unfolded(acc_ref):
    turned = acc_ref[...].T
    low = turned[0:ROWS] + turned[ROWS : 2 * ROWS]
    high = turned[2 * ROWS : 3 * ROWS] + turned[3 * ROWS : 4 * ROWS]
    return low, high


def device_of(bucket, z):
    zd, y, core = bucket // 8, (bucket // 2) % 4, bucket % 2
    return ((z // 2) * 2 + zd % 2) * 8 + y * 2 + core, zd // 2


def slots_of(z, y, core, x):
    return core * 128 + x * 32 + y * 8 + z, core * 128 + y * 32 + x * 8 + z


def slot_of_camera(d, g):
    zd = d // 8
    return slots_of(2 * g + zd % 2, (d // 2) % 4, d % 2, zd // 2)


def at(z, y, core, x):
    return (z * 8 + y * 2 + core, x)


def remote(src, dst, send, recv, device):
    return pltpu.make_async_remote_copy(
        src_ref=src, dst_ref=dst, send_sem=send, recv_sem=recv, device_id=device, device_id_type=MESH
    )


def looped(start, stop, do):
    def body(i, c):
        do(i)
        return c

    lax.fori_loop(start, stop, body, 0)


def camera_ids_here(cam_map, hot):
    slots = slots_of(*place())
    bases = (slots[0] * 128, (SLOTS + slots[1]) * 128)
    lane = lax.broadcasted_iota(jnp.int32, (1, 128), 1)
    rows = lax.broadcasted_iota(jnp.int32, (16, 128), 0)
    chunk = 16

    def body(i, acc):
        left, right = [], []
        for k in range(chunk):
            r = i * chunk + k
            cam = r * 128 + lane
            first = cam_map[pl.ds(r, 1), :] - bases[0]
            second = cam_map[pl.ds(r, 1), :] - bases[1]
            inside = jnp.where((first >= 0) & (first < 128), first, -16)
            inside = jnp.where((second >= 0) & (second < 128), second + 128, inside)
            hit = rows == (inside >> 4)
            left.append(
                jnp.concatenate(
                    [jnp.where(hit, (cam >> 8).astype(F32), 0.0), jnp.where(hit, (cam & 255).astype(F32), 0.0)], axis=0
                )
            )
            right.append(jnp.where(rows == (inside & 15), 1.0, 0.0))
        a = jnp.concatenate(left, axis=1).astype(BF16)
        b = jnp.concatenate(right, axis=1).astype(BF16)
        return acc + lax.dot_general(a, b, (((1,), (1,)), ((), ())), preferred_element_type=F32)

    acc = lax.fori_loop(0, 512 // chunk, body, jnp.zeros((32, 16), F32))
    cam = (acc[0:16] * 256.0 + acc[16:32]).astype(jnp.int32) & (256 * SLOTS - 1)
    d, g, h, lane = cam >> 10, (cam >> 8) & 3, (cam >> 7) & 1, cam & 127
    zd, y, core = d >> 3, (d >> 1) & 3, d & 1
    slots = slots_of(2 * g + (zd & 1), y, core, zd >> 1)
    spot = jnp.where(h == 0, slots[0], SLOTS + slots[1])
    spot = jnp.where(d == hot, 2 * SLOTS + 2 * g + h, spot)
    return spot * 128 + lane


def sum_buckets(
    counts, loads, jac, res, cam, cam_map, part_b, part_g, part_e, inv, msg, hots, gothot, acc, ssem, rsem, hssem, hrsem, gots
):
    chunk = 64 // len(gots)
    z, y, core, x = place()
    me = bucket_of(z, y, core, x)
    barrier = pltpu.get_barrier_semaphore()
    looped(
        1,
        64,
        lambda i: pl.semaphore_signal(
            barrier, inc=1, device_id=device_of((me + i) % 64, z), device_id_type=MESH
        ),
    )
    outside = [at(((z // 2) * 2 + i) % 8, y, core, x) for i in range(2, 8)]
    for peer in outside:
        pl.semaphore_signal(barrier, inc=1, device_id=peer, device_id_type=MESH)
    for c in loads:
        c.wait()
    lane = lax.broadcasted_iota(jnp.int32, (1, 128), 1)

    def pack(d, carry):
        hot, ejac, eres, eids = carry
        live = counts[0, d]
        for h in range(2):
            col = pl.multiple_of(d * CAP + h * 128, 128)
            msg[d, h, 0:18, :] = jac[:, pl.ds(col, 128)]
            msg[d, h, 18:20, :] = res[:, pl.ds(col, 128)]
            ids = cam[pl.ds(d * 4 + h, 1), :]
            msg[d, h, 20:21, :] = jnp.where(lane + h * 128 < live, ids, -1).astype(F32)
        full = live == CAP
        col = pl.multiple_of(d * CAP + 256, 128)
        ids = jnp.concatenate([cam[pl.ds(d * 4 + 2, 1), :], cam[pl.ds(d * 4 + 3, 1), :]], axis=1)
        return (
            jnp.where(full, d, hot),
            jnp.where(full, jac[:, pl.ds(col, 256)], ejac),
            jnp.where(full, res[:, pl.ds(col, 256)], eres),
            jnp.where(full, ids, eids),
        )

    hot, ejac, eres, eids = lax.fori_loop(
        0,
        64,
        pack,
        (jnp.int32(0), jnp.zeros((18, 256), F32), jnp.zeros((2, 256), F32), jnp.zeros((1, 256), jnp.int32)),
    )
    pl.semaphore_wait(barrier, 63 + len(outside))

    order = [(11 * k) % 64 for k in range(1, 64)]
    window = 24

    def copy(k):
        to = (me + order[k]) % 64
        return remote(msg.at[to], gots[k // chunk].at[k % chunk], ssem.at[k], rsem.at[k], device_of(to, z))

    def push(c):
        for k in range(c * chunk, min(c * chunk + chunk, 63)):
            if k >= window:
                copy(k - window).wait_send()
            copy(k).start()

    def hot_copy(i):
        to = (me + i) % 64
        return remote(hots.at[to], gothot.at[i], hssem.at[i], hrsem.at[i], device_of(to, z))

    for c in range(window // chunk):
        push(c)
    gots[-1][chunk - 1] = msg[me]
    acc[:, 4 * ROWS :] = jnp.zeros((HALF, 256 - 4 * ROWS), F32)
    acc[:, : 4 * ROWS] = weighted(ejac, eres, eids.astype(F32))
    low, high = unfolded(acc)
    for q in range(4):
        hots[0:ROWS, q, :] = low[:, q * 128 : (q + 1) * 128]
        hots[0:ROWS, 4 + q, :] = high[:, q * 128 : (q + 1) * 128]
    hots[ROWS:64] = jnp.zeros((64 - ROWS, 8, 128), F32)
    gothot[0] = hots[me]
    push(3)
    inv[...] = jnp.zeros_like(inv)
    inv[:, 0:16] = camera_ids_here(cam_map, hot)
    inv[0:1, 16:17] = jnp.full((1, 1), hot, jnp.int32)
    push(4)

    acc[...] = jnp.zeros_like(acc)
    for c in range(64 // chunk):
        for k in range(c * chunk, min(c * chunk + chunk, 63)):
            copy(k).wait_recv()
        whole = jnp.concatenate([gots[c][s, h] for s in range(chunk) for h in range(2)], axis=1)
        acc[:, : 4 * ROWS] += weighted(whole[0:18], whole[18:20], whole[20:21])
        if c < 3:
            push(5 + c)
        if c == 2:
            for i in range(1, 64):
                hot_copy(i).start()
    low, high = unfolded(acc)
    for i in range(1, 64):
        hot_copy(i).wait_recv()
    extra = jnp.sum(gothot[...], axis=0)
    for g in range(4):
        part = low if g < 2 else high
        for h in range(2):
            q = (g % 2) * 2 + h
            tile = part[:, q * 128 : (q + 1) * 128]
            part_b[g, h] = tile[0:48]
            part_g[g, h] = tile[48:56]
            part_e[g, h, 0:1] = tile[47:48]
            part_e[g, h, 1:2] = extra[g * 2 + h : g * 2 + h + 1]

    def finish():
        for k in range(63 - window, 63):
            copy(k).wait_send()
        for i in range(1, 64):
            hot_copy(i).wait_send()

    return finish


class Gather:
    def __init__(self, refs, sems):
        self.refs, self.sems = refs, sems
        z, y, core, x = place()
        self.slots = slots_of(z, y, core, x)
        ys = [at(z, (y + i) % 4, core, x) for i in range(1, 4)]
        xs = [at(z, y, core, (x + i) % 4) for i in range(1, 4)]
        self.zs = [at((z + i) % 8, y, core, x) for i in (4, 3, 5, 2, 6, 1, 7)]
        self.other = at(z, y, 1 - core, x)
        self.middle, self.last = (ys, xs), (xs, ys)
        self.mid, self.far = (y, x), (x, y)
        self.core = core

    def peers(self):
        return self.zs + self.middle[0] + self.middle[1] + [self.other]

    def copies(self, part, start, size, sem, device):
        out = []
        for n, ref in enumerate(self.refs):
            view = ref.at[pl.ds(part * SLOTS + start, size)]
            send, recv = self.sems[n]
            out.append(remote(view, view, send.at[part, sem], recv.at[part, sem], device))
        return out

    def start(self, *args):
        for c in self.copies(*args):
            c.start()

    def wait_recv(self, *args):
        for c in self.copies(*args):
            c.wait_recv()

    def run(self, between=()):
        between = list(between) + [lambda: None] * 4
        for part in range(2):
            for peer in self.zs:
                self.start(part, self.slots[part], 1, 0, peer)
        between[0]()
        blocks = [self.slots[part] // 8 * 8 for part in range(2)]
        for part in range(2):
            self.wait_recv(part, 0, 7, 0, self.zs[0])
            for i in (1, 0, 2):
                self.start(part, blocks[part], 8, 1 + i, self.middle[part][i])
            for i in (1, 0, 2):
                self.start(part, blocks[part], 8, 4 + i, self.last[part][i])
            self.start(part, blocks[part], 8, 7, self.other)
        between[1]()
        for i in (0, 2, 1):
            for part in range(2):
                base = self.core * 128 + self.far[part] * 32 + (self.mid[part] + 3 - i) % 4 * 8
                self.wait_recv(part, base, 8, 1 + i, self.middle[part][i])
                for j in (1, 0, 2):
                    self.start(part, base, 8, 4 + j, self.last[part][j])
                self.start(part, base, 8, 7, self.other)
        between[2]()
        for j in (0, 2, 1):
            for part in range(2):
                base = self.core * 128 + (self.far[part] + 3 - j) % 4 * 32
                self.wait_recv(part, base, 32, 4 + j, self.last[part][j])
                self.start(part, base, 32, 7, self.other)
        between[3]()
        for part in range(2):
            self.wait_recv(part, 0, 128, 7, self.other)

    def finish(self):
        for part in range(2):
            for sem, size in [(0, 7)] + [(k, 8) for k in (1, 2, 3)] + [(k, 32) for k in (4, 5, 6)] + [(7, 128)]:
                for c in self.copies(part, 0, size, sem, self.other):
                    c.wait_send()


def main_kernel(
    counts, jac_far, res_far, cam_far, map_far, table, table_e, blocks,
    jac, res, cam, cam_map, lsem,
    part_b, part_g, part_e, found, inv, msg, hots, gothot, acc, ssem, rsem, hssem, hrsem, isem,
    got_b, got_g, got_e, mine_b, bx, bz, grad, grad_e,
    s2b, r2b, s2g, r2g, s2e, r2e, sx, rx, sz, rz, sg, rg, se, re, sg2, rg2, se2, re2,
    *gots,
):
    far = ((jac_far, jac), (res_far, res), (cam_far, cam), (map_far, cam_map))
    loads = [pltpu.make_async_copy(*pair, lsem.at[n]) for n, pair in enumerate(far)]
    for c in loads:
        c.start()
    sums_sent = sum_buckets(
        counts, loads, jac, res, cam, cam_map, part_b, part_g, part_e, found, msg, hots, gothot, acc, ssem, rsem, hssem, hrsem, gots
    )
    z, y, core, x = place()
    g, p = z // 2, z % 2
    first = Gather((grad, grad_e), ((sg, rg), (se, re)))
    second = Gather((table, table_e), ((sg2, rg2), (se2, re2)))
    ids = pltpu.make_async_copy(found, inv, isem)
    ids.start()

    small, large = [], []
    for i in range(1, 4):
        to = (g + i) % 4
        device = at(2 * to + p, y, core, x)
        small.append(remote(part_g.at[to], got_g.at[i - 1], s2g.at[i - 1], r2g.at[i - 1], device))
        small.append(remote(part_e.at[to], got_e.at[i - 1], s2e.at[i - 1], r2e.at[i - 1], device))
        large.append(remote(part_b.at[to], got_b.at[i - 1], s2b.at[i - 1], r2b.at[i - 1], device))
    for c in small:
        c.start()
    for c in small:
        c.wait_recv()
    total_g = part_g[g] + got_g[0] + got_g[1] + got_g[2]
    total_e = part_e[g] + got_e[0] + got_e[1] + got_e[2]
    for h in range(2):
        grad[h * SLOTS + first.slots[h]] = total_g[h]
        grad_e[h * SLOTS + first.slots[h]] = total_e[h]

    across, along = [], []
    for i in range(1, 4):
        across.append(remote(mine_b, bx.at[x], sx.at[i - 1], rx.at[i - 1], at(z, y, core, (x + i) % 4)))
        to = (g + i) % 4
        along.append(remote(bx.at[to], bz.at[g], sz.at[i - 1], rz.at[i - 1], at(2 * to + p, y, core, x)))

    def nothing():
        pass

    def start_blocks():
        for c in large:
            c.start()

    def spread_blocks():
        for c in large:
            c.wait_recv()
        mine_b[...] = part_b[g] + got_b[0] + got_b[1] + got_b[2]
        bx[x] = mine_b[...]
        for c in across:
            c.start()

    def send_blocks():
        for c in across:
            c.wait_recv()
        for c in along:
            c.start()
        bz[g] = bx[g]

    first.run([nothing, start_blocks])

    ids.wait()
    hot = inv[0, 16]
    for gg in range(4):
        hot_slots = slot_of_camera(hot, gg)
        for h in range(2):
            slot = h * SLOTS + hot_slots[h]
            extra = [grad_e[h * SLOTS + slot_of_camera(48 + k, gg)[h], 1:2] for k in range(8)]
            grad[2 * SLOTS + 2 * gg + h] = grad[slot] + jnp.concatenate(extra, axis=0)
            grad_e[2 * SLOTS + 2 * gg + h, 0:1] = (
                grad_e[slot, 0:1] + grad_e[h * SLOTS + slot_of_camera(47, gg)[h], 1:2]
            )
            grad_e[2 * SLOTS + 2 * gg + h, 1:2] = jnp.zeros((1, 128), F32)
    lane = lax.broadcasted_iota(jnp.int32, (1, 128), 1)
    for h in range(2):

        def pick(r, acc):
            top, low = acc
            for k in range(64):
                v = inv[h * 8 + r * 4 + k // 16, k % 16]
                q = r * 64 + k
                turn = (q - v) & 127
                at_q = lane == q
                top = jnp.where(at_q, pltpu.roll(grad[v >> 7], turn, 1), top)
                low = jnp.where(at_q, pltpu.roll(grad_e[v >> 7], turn, 1), low)
            return top, low

        top, low = lax.fori_loop(0, 2, pick, (jnp.zeros((8, 128), F32), jnp.zeros((2, 128), F32)))
        table[h * SLOTS + second.slots[h]] = top
        table_e[h * SLOTS + second.slots[h]] = low[0:1]

    def fix_blocks():
        for c in along:
            c.wait_recv()
        here = lax.axis_index("obs") == hot
        for gg in range(4):
            for h in range(2):
                extra = [grad_e[h * SLOTS + slot_of_camera(t, gg)[h], 1:2] for t in range(45)]
                extra = jnp.concatenate(extra + [jnp.zeros((3, 128), F32)], axis=0)
                blocks[gg, h] = bz[gg, h] + jnp.where(here, extra, 0.0)

    second.run([spread_blocks, send_blocks, nothing, fix_blocks])
    for c in small + large + across + along:
        c.wait_send()
    first.finish()
    second.finish()
    sums_sent()


def finish_kernel(table, table_e, blocks, out, blocks_out):
    for n in range(table.shape[0]):
        out[0:8, n * 128 : (n + 1) * 128] = table[n]
        out[8:9, n * 128 : (n + 1) * 128] = table_e[n]
    whole = blocks[0, 0]
    for k in range(9):
        for j in range(5):
            m = (k + j) % 9
            t = 40 + j if k == 8 else j * 8 + k
            blocks_out[k * 9 + m : k * 9 + m + 1, :] = whole[t : t + 1]
            if j:
                blocks_out[m * 9 + k : m * 9 + k + 1, :] = whole[t : t + 1]


def shape(*dims, dtype=F32):
    return jax.ShapeDtypeStruct(dims, dtype)


def call(kernel, out, ins, scratch=(), cid=None, **kw):
    params = dict(vmem_limit_bytes=60 * 1024 * 1024)
    if cid is not None:
        params.update(collective_id=cid, has_side_effects=True)
    many = isinstance(out, tuple)
    return pl.pallas_call(
        kernel,
        out_shape=out,
        in_specs=ins,
        out_specs=tuple(VM() for _ in out) if many else VM(),
        scratch_shapes=list(scratch),
        compiler_params=pltpu.CompilerParams(**params),
        **kw,
    )


def vmem(*dims):
    return pltpu.VMEM(dims, F32)


def local(jacobians, residuals, camera_local, bucket_counts, camera_map):
    dma = pltpu.SemaphoreType.DMA
    table, table_e, blocks = call(
        main_kernel,
        (shape(2 * SLOTS, 8, 128), shape(2 * SLOTS, 1, 128), shape(4, 2, 48, 128)),
        [SM()] + [pl.BlockSpec(memory_space=pl.ANY)] * 4,
        [
            vmem(18, 32768),
            vmem(2, 32768),
            pltpu.VMEM((256, 128), jnp.int32),
            pltpu.VMEM((512, 128), jnp.int32),
            dma((4,)),
            vmem(4, 2, 48, 128),
            vmem(4, 2, 8, 128),
            vmem(4, 2, 2, 128),
            pltpu.VMEM((16, 128), jnp.int32),
            pltpu.SMEM((16, 128), jnp.int32),
            vmem(64, 2, MSG, 128),
            vmem(64, 8, 128),
            vmem(64, 8, 128),
            vmem(HALF, 256),
        ]
        + [dma((64,))] * 4
        + [
            dma,
            vmem(3, 2, 48, 128),
            vmem(3, 2, 8, 128),
            vmem(3, 2, 2, 128),
            vmem(2, 48, 128),
            vmem(4, 2, 48, 128),
            vmem(4, 2, 48, 128),
            vmem(2 * SLOTS + 8, 8, 128),
            vmem(2 * SLOTS + 8, 2, 128),
        ]
        + [dma((3,))] * 10
        + [dma((2, 8))] * 8
        + [vmem(8, 2, MSG, 128)] * 8,
        cid=1,
        name="main",
    )(bucket_counts, jacobians, residuals, camera_local.reshape(256, 128), camera_map.reshape(512, 128))
    return pl.pallas_call(
        finish_kernel,
        out_shape=(shape(9, 65536), shape(81, 1024)),
        grid=(8,),
        in_specs=[
            pl.BlockSpec((2 * SLOTS // 8, 8, 128), lambda n: (n, 0, 0)),
            pl.BlockSpec((2 * SLOTS // 8, 1, 128), lambda n: (n, 0, 0)),
            pl.BlockSpec((1, 1, 48, 128), lambda n: (n // 2, n % 2, 0, 0)),
        ],
        out_specs=(pl.BlockSpec((9, 8192), lambda n: (0, n)), pl.BlockSpec((81, 128), lambda n: (0, n))),
        name="finish",
    )(table, table_e, blocks)


def solution(mesh):
    return jax.shard_map(
        local,
        mesh=mesh,
        in_specs=(P(None, ("obs", "rep")), P(None, ("obs", "rep")), P(("obs", "rep")), P(("obs", "rep"), None), P()),
        out_specs=(P(), P(None, "obs")),
        check_vma=False,
    )
```
